128 devices in a mesh: data: 128 (over z, y, x, core).
Axes of the slice: x: 4, y: 4, z: 4, core: 2. Of those that a mesh axis runs over, the one named last changes fastest.
Arguments:
- x_tokens: bfloat16 [262144, 768], P('data')
- dh_out: bfloat16 [262144, 768], P('data')
- w_up: bfloat16 [2, 768, 2048], replicated
- w_down: bfloat16 [2, 2048, 768], replicated
- proj_up: bfloat16 [2, 768, 256], replicated
- proj_down: bfloat16 [2, 768, 256], replicated
- mom_up: float32 [2, 256, 2048], P(None, None, 'data')
- var_up: float32 [2, 256, 2048], P(None, None, 'data')
- mom_down: float32 [2, 2048, 256], P(None, 'data')
- var_down: float32 [2, 2048, 256], P(None, 'data')
Outputs:
- output 1: bfloat16 [2, 768, 2048], replicated
- output 2: bfloat16 [2, 2048, 768], replicated
- output 3: float32 [2, 256, 2048], P(None, None, 'data')
- output 4: float32 [2, 256, 2048], P(None, None, 'data')
- output 5: float32 [2, 2048, 256], P(None, 'data')
- output 6: float32 [2, 2048, 256], P(None, 'data')
All inputs are finite; a program needn't handle non-finite values.
Results may differ from the reference program's by a relative error of at most 0.0072576.
Values are sent between devices in bfloat16 or wider.
A program may use at most 1 GiB of HBM per device.

```python
import jax
import jax.numpy as jnp
from jax import lax

D = 768
FF = 2048
RANK = 256
TOKENS = 262144
BLOCK = 1024
STEP = 4
BETA_ONE = 0.9
BETA_TWO = 0.999
EPSILON = 1e-8
LEARN_RATE = 0.02
ALPHA_SCALE = 0.25


def setup_inputs(seed: int = 0) -> dict:
    key_list = jax.random.split(jax.random.key(seed), 10)
    x_tokens = jax.random.normal(key_list[0], (TOKENS, D), jnp.float32)
    dh_out = jax.random.normal(key_list[1], (TOKENS, D), jnp.float32) * (20.0 * TOKENS ** -0.5)
    w_up = jax.random.normal(key_list[2], (2, D, FF), jnp.float32) * D ** -0.5
    w_down = jax.random.normal(key_list[3], (2, FF, D), jnp.float32) * FF ** -0.5
    proj_up = jnp.linalg.qr(jax.random.normal(key_list[4], (2, D, RANK), jnp.float32))[0]
    proj_down = jnp.linalg.qr(jax.random.normal(key_list[5], (2, D, RANK), jnp.float32))[0]
    mom_up = jax.random.normal(key_list[6], (2, RANK, FF), jnp.float32)
    var_up = jax.random.uniform(key_list[7], (2, RANK, FF), jnp.float32, 0.05, 0.15)
    mom_down = jax.random.normal(key_list[8], (2, FF, RANK), jnp.float32)
    var_down = jax.random.uniform(key_list[9], (2, FF, RANK), jnp.float32, 0.05, 0.15)
    return {
        'x_tokens': x_tokens.astype(jnp.bfloat16),
        'dh_out': dh_out.astype(jnp.bfloat16),
        'w_up': w_up.astype(jnp.bfloat16),
        'w_down': w_down.astype(jnp.bfloat16),
        'proj_up': proj_up.astype(jnp.bfloat16),
        'proj_down': proj_down.astype(jnp.bfloat16),
        'mom_up': mom_up,
        'var_up': var_up,
        'mom_down': mom_down,
        'var_down': var_down,
    }


def block_grads(x_rows, dh_rows, w_up, w_down, proj_up, proj_down):
    hidden = [x_rows]
    act_list = []
    pull_list = []
    for layer_idx in range(2):
        pre_act = jnp.dot(hidden[layer_idx], w_up[layer_idx], preferred_element_type=jnp.float32)
        gelu_val, gelu_pull = jax.vjp(jax.nn.gelu, pre_act)
        act_val = gelu_val.astype(jnp.bfloat16)
        down_out = jnp.dot(act_val, w_down[layer_idx], preferred_element_type=jnp.float32)
        hidden.append((hidden[layer_idx].astype(jnp.float32) + down_out).astype(jnp.bfloat16))
        act_list.append(act_val)
        pull_list.append(gelu_pull)
    grad_rows = dh_rows
    up_parts = [None, None]
    down_parts = [None, None]
    for layer_idx in (1, 0):
        v_proj = jnp.dot(grad_rows, proj_down[layer_idx], preferred_element_type=jnp.float32).astype(jnp.bfloat16)
        down_parts[layer_idx] = jnp.dot(act_list[layer_idx].T, v_proj, preferred_element_type=jnp.float32)
        d_act = jnp.dot(grad_rows, w_down[layer_idx].T, preferred_element_type=jnp.float32)
        d_pre = pull_list[layer_idx](d_act)[0].astype(jnp.bfloat16)
        u_proj = jnp.dot(hidden[layer_idx], proj_up[layer_idx], preferred_element_type=jnp.float32).astype(jnp.bfloat16)
        up_parts[layer_idx] = jnp.dot(u_proj.T, d_pre, preferred_element_type=jnp.float32)
        if layer_idx > 0:
            back_term = jnp.dot(d_pre, w_up[layer_idx].T, preferred_element_type=jnp.float32)
            grad_rows = (grad_rows.astype(jnp.float32) + back_term).astype(jnp.bfloat16)
    return jnp.stack(up_parts), jnp.stack(down_parts)


def adam_step(moment, variance, grad_red):
    new_mom = BETA_ONE * moment + (1.0 - BETA_ONE) * grad_red
    new_var = BETA_TWO * variance + (1.0 - BETA_TWO) * grad_red * grad_red
    bias_one = 1.0 - BETA_ONE ** STEP
    bias_two = 1.0 - BETA_TWO ** STEP
    direction = (new_mom / bias_one) / (jnp.sqrt(new_var / bias_two) + EPSILON)
    return new_mom, new_var, direction.astype(jnp.bfloat16)


def reference(x_tokens, dh_out, w_up, w_down, proj_up, proj_down, mom_up, var_up, mom_down, var_down):
    x_blocks = x_tokens.reshape(TOKENS // BLOCK, BLOCK, D)
    dh_blocks = dh_out.reshape(TOKENS // BLOCK, BLOCK, D)

    def scan_body(carry_acc, block_pair):
        part_up, part_down = block_grads(block_pair[0], block_pair[1], w_up, w_down, proj_up, proj_down)
        return (carry_acc[0] + part_up, carry_acc[1] + part_down), None

    zero_init = (jnp.zeros((2, RANK, FF), jnp.float32), jnp.zeros((2, FF, RANK), jnp.float32))
    scan_out = lax.scan(scan_body, zero_init, (x_blocks, dh_blocks))
    red_up, red_down = scan_out[0]
    new_mom_up, new_var_up, dir_up = adam_step(mom_up, var_up, red_up)
    new_mom_down, new_var_down, dir_down = adam_step(mom_down, var_down, red_down)
    delta_up = jnp.einsum('ldr,lrf->ldf', proj_up.astype(jnp.float32), dir_up.astype(jnp.float32))
    delta_down = jnp.einsum('lfr,ldr->lfd', dir_down.astype(jnp.float32), proj_down.astype(jnp.float32))
    new_w_up = (w_up.astype(jnp.float32) - (LEARN_RATE * ALPHA_SCALE) * delta_up).astype(jnp.bfloat16)
    new_w_down = (w_down.astype(jnp.float32) - (LEARN_RATE * ALPHA_SCALE) * delta_down).astype(jnp.bfloat16)
    return (new_w_up, new_w_down, new_mom_up, new_var_up, new_mom_down, new_var_down)
```

```python
import jax
import jax.numpy as jnp
from jax import lax
from jax.experimental import pallas as pl
from jax.experimental.pallas import tpu as pltpu
from jax.sharding import PartitionSpec as P

BETA_ONE = 0.9
BETA_TWO = 0.999
EPSILON = 1e-8
STEP = 4
LEARN_RATE = 0.02
ALPHA_SCALE = 0.25
SCALE = LEARN_RATE * ALPHA_SCALE
MESH = pl.DeviceIdType.MESH

ORDERS = ((2, 1, 0), (1, 0, 2), (0, 2, 1))
GROUPS = (
    ((0, 0, 2), (1, 2, 1), (2, 3, 1)),
    ((0, 0, 1), (1, 1, 2), (2, 3, 1)),
    ((0, 0, 1), (1, 1, 1), (2, 2, 2)),
    ((0, 0, 2), (1, 2, 1), (2, 3, 1)),
)
UNITS = ((0, 1), (2, 0), (1, 2), (0, 1))


def contract_rows(lhs, rhs):
    return lax.dot_general(lhs, rhs, (((0,), (0,)), ((), ())), preferred_element_type=jnp.float32)


def contract_cols(lhs, rhs):
    return lax.dot_general(lhs, rhs, (((1,), (1,)), ((), ())), preferred_element_type=jnp.float32)


def local_grads(x_rows, dh_rows, w_up, w_down, proj_up, proj_down):
    layers = w_up.shape[0]
    hidden = [x_rows]
    act_list = []
    pull_list = []
    for layer_idx in range(layers):
        pre_act = jnp.dot(hidden[layer_idx], w_up[layer_idx], preferred_element_type=jnp.float32)
        gelu_val, gelu_pull = jax.vjp(jax.nn.gelu, pre_act)
        act_val = gelu_val.astype(jnp.bfloat16)
        if layer_idx + 1 < layers:
            down_out = jnp.dot(act_val, w_down[layer_idx], preferred_element_type=jnp.float32)
            hidden.append((hidden[layer_idx] + down_out).astype(jnp.bfloat16))
        act_list.append(act_val)
        pull_list.append(gelu_pull)
    grad_rows = dh_rows
    parts = [None] * (2 * layers)
    for layer_idx in reversed(range(layers)):
        v_proj = jnp.dot(grad_rows, proj_down[layer_idx], preferred_element_type=jnp.float32).astype(jnp.bfloat16)
        parts[2 * layer_idx + 1] = contract_rows(act_list[layer_idx], v_proj)
        d_act = contract_cols(grad_rows, w_down[layer_idx])
        d_pre = pull_list[layer_idx](d_act)[0].astype(jnp.bfloat16)
        u_proj = jnp.dot(hidden[layer_idx], proj_up[layer_idx], preferred_element_type=jnp.float32).astype(jnp.bfloat16)
        parts[2 * layer_idx] = contract_rows(d_pre, u_proj)
        if layer_idx > 0:
            grad_rows = (grad_rows + contract_cols(d_pre, w_up[layer_idx])).astype(jnp.bfloat16)
    return parts


def adam_shard(moment, variance, grad_red):
    new_mom = BETA_ONE * moment + (1.0 - BETA_ONE) * grad_red
    new_var = BETA_TWO * variance + (1.0 - BETA_TWO) * grad_red * grad_red
    bias_one = 1.0 - BETA_ONE ** STEP
    bias_two = 1.0 - BETA_TWO ** STEP
    direction = (new_mom / bias_one) / (jnp.sqrt(new_var / bias_two) + EPSILON)
    return new_mom, new_var, direction.astype(jnp.bfloat16)


class Torus:
    def __init__(self):
        me = lax.axis_index("data")
        self.core = lax.rem(me, 2)
        chip = me // 2
        self.coords = (chip // 16, lax.rem(chip // 4, 4), lax.rem(chip, 4))
        self.partner = me + 1 - 2 * self.core

    def coord(self, axis, offset):
        return lax.rem(self.coords[axis] + offset, 4)

    def peer(self, axis, offset):
        z, y, x = (self.coord(a, offset) if a == axis else self.coords[a] for a in range(3))
        return ((z * 4 + y) * 4 + x) * 2 + self.core


def remote(src, dst, send_sem, recv_sem, device):
    return pltpu.make_async_remote_copy(
        src_ref=src, dst_ref=dst, send_sem=send_sem, recv_sem=recv_sem,
        device_id=(device,), device_id_type=MESH,
    )


def entry_barrier(torus):
    barrier = pltpu.get_barrier_semaphore()
    pl.semaphore_signal(barrier, inc=1, device_id=(torus.partner,), device_id_type=MESH)
    for axis in range(3):
        for offset in (1, 2, 3):
            pl.semaphore_signal(barrier, inc=1, device_id=(torus.peer(axis, offset),), device_id_type=MESH)
    pl.semaphore_wait(barrier, 10)


def at_axis(axes, axis, index):
    return tuple(index if a == axis else slice(None) for a in axes)


def update_kernel(r0, r1, r2, r3, mom_ref, var_ref, dir_out, mom_out, var_out,
                  own, pair, rb1, part1, rb2, part2, rb3, red, gath,
                  load_sem, pair_send, pair_recv, rs_send, rs_recv, ag_send, ag_recv, swap_send, swap_recv, out_sem):
    torus = Torus()
    core = torus.core
    sources = (r0, r1, r2, r3)
    loads, swaps = [], []
    for m, src in enumerate(sources):
        for t in range(4):
            i, j = divmod(t, 2)
            cp = pltpu.make_async_copy(
                src.at[:, :, :, core, i, :, pl.ds(128 * j, 128)], own.at[m, t], load_sem.at[m, t])
            cp.start()
            loads.append(cp)
    entry_barrier(torus)
    for m, src in enumerate(sources):
        for t in range(4):
            i, j = divmod(t, 2)
            cp = remote(src.at[:, :, :, 1 - core, i, :, pl.ds(128 * j, 128)], pair.at[m, t],
                        pair_send.at[m, t], pair_recv.at[m, t], torus.partner)
            cp.start()
            swaps.append(cp)

    sends = list(swaps)
    recvs = {}

    def scatter(phase, m, colour, first, count):
        order = ORDERS[colour]
        axis = order[phase]
        axes = tuple(a for a in range(3) if a not in order[:phase])
        src = (own, part1, part2)[phase]
        dst = (rb1, rb2, rb3)[phase]
        slots = pl.ds(first, count)
        for offset in (1, 2, 3):
            where = at_axis(axes, axis, torus.coord(axis, offset))
            cp = remote(src.at[(m, slots) + where], dst.at[m, offset - 1, slots],
                        rs_send.at[phase, m, colour, offset - 1], rs_recv.at[phase, m, colour, offset - 1],
                        torus.peer(axis, offset))
            cp.start()
            sends.append(cp)
            recvs[phase, m, colour, offset] = cp

    def gather_sum(phase, m, colour, first, count):
        order = ORDERS[colour]
        axis = order[phase]
        axes = tuple(a for a in range(3) if a not in order[:phase])
        src = (own, part1, part2)[phase]
        got = (rb1, rb2, rb3)[phase]
        slots = pl.ds(first, count)
        for offset in (1, 2, 3):
            recvs[phase, m, colour, offset].wait_recv()
        mine = src[(m, slots) + at_axis(axes, axis, torus.coords[axis])]
        total = mine + got[m, 0, slots] + got[m, 1, slots] + got[m, 2, slots]
        if phase == 0:
            part1[m, slots] = total
        elif phase == 1:
            part2[m, slots] = total
        else:
            for k in range(count):
                i, j = divmod(first + k, 2)
                red[m, 8 * i:8 * i + 8, 128 * j:128 * j + 128] = total[k]

    for m in range(4):
        for t in range(4):
            loads[4 * m + t].wait()
            swaps[4 * m + t].wait_recv()

            def add_row(z, _, m=m, t=t):
                own[m, t, z] = own[m, t, z] + pair[m, t, z]
                return 0

            lax.fori_loop(0, 4, add_row, 0)
        for colour, first, count in GROUPS[m]:
            scatter(0, m, colour, first, count)
    for m in range(4):
        for colour, first, count in GROUPS[m]:
            gather_sum(0, m, colour, first, count)
            scatter(1, m, colour, first, count)
    for m in range(4):
        for colour, first, count in GROUPS[m]:
            gather_sum(1, m, colour, first, count)
            scatter(2, m, colour, first, count)

    ag = {}
    z, y, x = torus.coords

    def spread(phase, m, j):
        order = ORDERS[UNITS[m][j]][::-1]
        axis = order[phase]
        lanes = pl.ds(128 * j, 128)
        where = tuple(slice(None) if a in order[:phase] else torus.coords[a] for a in range(3))
        ref = gath.at[(m,) + where + (core, slice(None), lanes)]
        for offset in (1, 2, 3):
            cp = remote(ref, ref, ag_send.at[phase, m, j, offset - 1], ag_recv.at[phase, m, j, offset - 1],
                        torus.peer(axis, offset))
            cp.start()
            sends.append(cp)
            ag[phase, m, j, offset] = cp

    for m in range(4):
        for colour, first, count in GROUPS[m]:
            gather_sum(2, m, colour, first, count)
        new_mom, new_var, direction = adam_shard(mom_ref[m], var_ref[m], red[m])
        mom_out[m] = new_mom
        var_out[m] = new_var
        gath[m, z, y, x, core] = direction
        for j in range(2):
            spread(0, m, j)
    for phase in (0, 1):
        for m in range(4):
            for j in range(2):
                for offset in (1, 2, 3):
                    ag[phase, m, j, offset].wait_recv()
                spread(phase + 1, m, j)
    finals = []
    for m in range(4):
        for j in range(2):
            for offset in (1, 2, 3):
                ag[2, m, j, offset].wait_recv()
        ref = gath.at[m, :, :, :, core]
        cp = remote(ref, ref, swap_send.at[m], swap_recv.at[m], torus.partner)
        cp.start()
        finals.append(cp)
    outs = []
    for m in range(4):
        finals[m].wait_recv()
        cp = pltpu.make_async_copy(gath.at[m], dir_out.at[m], out_sem.at[m])
        cp.start()
        outs.append(cp)
    for cp in sends + finals:
        cp.wait_send()
    for cp in outs:
        cp.wait()


def reduce_update(parts, mom, var):
    f32, bf16 = jnp.float32, jnp.bfloat16
    dma = pltpu.SemaphoreType.DMA
    shard = jax.ShapeDtypeStruct((4, 16, 256), f32)
    return pl.pallas_call(
        update_kernel,
        out_shape=(jax.ShapeDtypeStruct((4, 4, 4, 4, 2, 16, 256), bf16), shard, shard),
        in_specs=[pl.BlockSpec(memory_space=pl.ANY)] * 4 + [pl.BlockSpec(memory_space=pltpu.VMEM)] * 2,
        out_specs=(pl.BlockSpec(memory_space=pl.ANY),) + (pl.BlockSpec(memory_space=pltpu.VMEM),) * 2,
        scratch_shapes=[
            pltpu.VMEM((4, 4, 4, 4, 4, 8, 128), f32),
            pltpu.VMEM((4, 4, 4, 4, 4, 8, 128), f32),
            pltpu.VMEM((4, 3, 4, 4, 4, 8, 128), f32),
            pltpu.VMEM((4, 4, 4, 4, 8, 128), f32),
            pltpu.VMEM((4, 3, 4, 4, 8, 128), f32),
            pltpu.VMEM((4, 4, 4, 8, 128), f32),
            pltpu.VMEM((4, 3, 4, 8, 128), f32),
            pltpu.VMEM((4, 16, 256), f32),
            pltpu.VMEM((4, 4, 4, 4, 2, 16, 256), bf16),
            dma((4, 4)), dma((4, 4)), dma((4, 4)),
            dma((3, 4, 3, 3)), dma((3, 4, 3, 3)),
            dma((3, 4, 2, 3)), dma((3, 4, 2, 3)),
            dma((4,)), dma((4,)), dma((4,)),
        ],
        compiler_params=pltpu.CompilerParams(collective_id=0, has_side_effects=True),
    )(*[p.reshape(4, 4, 4, 2, 2, 8, 256) for p in parts], mom, var)


def solution(mesh):
    def local_step(x_loc, dh_loc, w_up, w_down, proj_up, proj_down, mom_up, var_up, mom_down, var_down):
        parts = local_grads(x_loc, dh_loc, w_up, w_down, proj_up, proj_down)

        def pack(up, down):
            up = jnp.swapaxes(up, 1, 2)
            return jnp.stack([up[0], down[0], up[1], down[1]])

        directions, new_mom, new_var = reduce_update(parts, pack(mom_up, mom_down), pack(var_up, var_down))
        directions = directions.reshape(4, 2048, 256)
        dir_up, dir_down = directions[0::2], directions[1::2]
        delta_up = jnp.einsum('ldr,lfr->ldf', proj_up, dir_up, preferred_element_type=jnp.float32)
        delta_down = jnp.einsum('lfr,ldr->lfd', dir_down, proj_down, preferred_element_type=jnp.float32)
        new_w_up = (w_up - SCALE * delta_up).astype(jnp.bfloat16)
        new_w_down = (w_down - SCALE * delta_down).astype(jnp.bfloat16)
        return (new_w_up, new_w_down,
                jnp.swapaxes(new_mom[0::2], 1, 2), jnp.swapaxes(new_var[0::2], 1, 2), new_mom[1::2], new_var[1::2])

    tok_spec = P('data', None)
    up_spec = P(None, None, 'data')
    down_spec = P(None, 'data', None)
    return jax.shard_map(
        local_step,
        mesh=mesh,
        in_specs=(tok_spec, tok_spec, P(), P(), P(), P(), up_spec, up_spec, down_spec, down_spec),
        out_specs=(P(), P(), up_spec, up_spec, down_spec, down_spec),
        check_vma=False,
    )
```

```python
import jax
import jax.numpy as jnp
from jax import lax
from jax.experimental import pallas as pl
from jax.experimental.pallas import tpu as pltpu
from jax.sharding import PartitionSpec as P

BETA_ONE = 0.9
BETA_TWO = 0.999
EPSILON = 1e-8
STEP = 4
LEARN_RATE = 0.02
ALPHA_SCALE = 0.25
SCALE = LEARN_RATE * ALPHA_SCALE
GELU_A = 0.7978845608028654
GELU_B = 0.044715
MESH = pl.DeviceIdType.MESH
F32, BF16 = jnp.float32, jnp.bfloat16

BLOCK = 512
TILE = 256
BLOCKS = 4
TILES = 8

ORDERS = ((2, 1, 0), (1, 0, 2), (0, 2, 1))
COLOURS = ((0, 1, 2), (1, 2, 0), (2, 0, 1), (0, 1, 2))
PIECES = ((0, 0, 256), (1, 0, 128), (1, 128, 128))
UNITS = ((0, 1), (2, 0), (1, 2), (0, 1))


def dot(lhs, rhs):
    return jnp.dot(lhs, rhs, preferred_element_type=F32)


def dot_t(lhs, rhs):
    return lax.dot_general(lhs, rhs, (((1,), (1,)), ((), ())), preferred_element_type=F32)


def gelu_pair(z):
    sq = z * z
    cdf = 0.5 + 0.5 * jnp.tanh(z * (GELU_A + (GELU_A * GELU_B) * sq))
    act = z * cdf
    slope = cdf + act * ((1.0 - cdf) * (2.0 * GELU_A + (6.0 * GELU_A * GELU_B) * sq))
    return act, slope


def adam_shard(moment, variance, grad_red):
    new_mom = BETA_ONE * moment + (1.0 - BETA_ONE) * grad_red
    new_var = BETA_TWO * variance + (1.0 - BETA_TWO) * grad_red * grad_red
    bias_one = 1.0 - BETA_ONE ** STEP
    bias_two = 1.0 - BETA_TWO ** STEP
    direction = (new_mom / bias_one) / (jnp.sqrt(new_var / bias_two) + EPSILON)
    return new_mom, new_var, direction.astype(BF16)


def block_rows(i):
    return pl.ds(pl.multiple_of(i * BLOCK, BLOCK), BLOCK)


def tile_cols(n):
    return pl.ds(pl.multiple_of(n * TILE, TILE), TILE)


def grad_kernel(x_hbm, dh_hbm, wu_hbm, wd_hbm, pu_hbm, pd_hbm, r_out, gp_hbm,
                h, g, wu, wd, pu, pd, act, dz, ut0, ut1, vt, gp, tile, rtmp, in_sem, gp_sem, r_sem):
    loads = {}

    def load(name, src, dst):
        cp = pltpu.make_async_copy(src, dst, in_sem.at[len(loads)])
        cp.start()
        loads[name] = cp

    load("x", x_hbm, h)
    load("wu0", wu_hbm.at[0], wu.at[0])
    load("pu", pu_hbm, pu)
    load("wd0", wd_hbm.at[0], wd.at[0])
    load("dh", dh_hbm, g)
    load("pd", pd_hbm, pd)
    load("wu1", wu_hbm.at[1], wu.at[1])
    load("wd1", wd_hbm.at[1], wd.at[1])

    def slope_out(rb):
        return pltpu.make_async_copy(gp, gp_hbm.at[:, rb], gp_sem.at[0])

    def slope_in(n, half):
        return pltpu.make_async_copy(gp_hbm.at[n], gp.at[pl.ds(4 * half, 4)], gp_sem.at[half])

    def emit_copy(m, n, slot):
        return pltpu.make_async_copy(
            rtmp.at[slot], r_out.at[m, n // 2, pl.ds(2 * lax.rem(n, 2), 2)], r_sem.at[slot])

    def emit(m, n, slot, part):
        rtmp[slot] = part.T.reshape(2, 4, 2, 2, 8, 256)
        emit_copy(m, n, slot).start()

    for name in ("x", "wu0", "pu", "wd0"):
        loads[name].wait()

    def forward_zero(rb, _):
        rows = block_rows(rb)
        hidden = h[rows]
        ut0[:, rows] = dot(hidden, pu[0]).astype(BF16).T
        for n in range(TILES):
            cols = slice(TILE * n, TILE * n + TILE)
            value, slope = gelu_pair(dot(hidden, wu[0, :, cols]))
            act[rows, cols] = value.astype(BF16)
            gp[n] = slope
        cp = slope_out(rb)
        cp.start()
        h[rows] = (hidden + dot(act[rows], wd[0])).astype(BF16)
        cp.wait()
        return 0

    lax.fori_loop(0, BLOCKS, forward_zero, 0)
    for name in ("dh", "pd", "wu1", "wd1"):
        loads[name].wait()

    def project_one(rb, _):
        rows = block_rows(rb)
        ut1[:, rows] = dot(h[rows], pu[1]).astype(BF16).T
        vt[:, rows] = dot(g[rows], pd[1]).astype(BF16).T
        return 0

    lax.fori_loop(0, BLOCKS, project_one, 0)

    def layer_one(n, _):
        cols = tile_cols(n)
        slot = 2 * lax.rem(n, 2)

        @pl.when(n >= 2)
        def _():
            emit_copy(3, n - 2, slot).wait()
            emit_copy(2, n - 2, slot + 1).wait()

        for rc in range(BLOCKS):
            rows = slice(BLOCK * rc, BLOCK * rc + BLOCK)
            value, slope = gelu_pair(dot(h[rows], wu[1, :, cols]))
            tile[rows] = value.astype(BF16)
            dz[rows, cols] = (slope * dot_t(g[rows], wd[1, cols, :])).astype(BF16)
        emit(3, n, slot, dot(vt[...], tile[...]))
        emit(2, n, slot + 1, dot(ut1[...], dz[:, cols]))
        return 0

    lax.fori_loop(0, TILES, layer_one, 0)
    slope_in(0, 0).start()

    def input_grad(rb, _):
        rows = block_rows(rb)
        grad = (g[rows] + dot_t(dz[rows], wu[1])).astype(BF16)
        g[rows] = grad
        vt[:, rows] = dot(grad, pd[0]).astype(BF16).T
        return 0

    lax.fori_loop(0, BLOCKS, input_grad, 0)
    for n in (TILES - 2, TILES - 1):
        emit_copy(3, n, 2 * (n % 2)).wait()
        emit_copy(2, n, 2 * (n % 2) + 1).wait()

    def down_zero(n, _):
        slot = lax.rem(n, 2)

        @pl.when(n >= 2)
        def _():
            emit_copy(1, n - 2, slot).wait()

        emit(1, n, slot, dot(vt[...], act[:, tile_cols(n)]))
        return 0

    lax.fori_loop(0, TILES, down_zero, 0)

    def up_zero(n, _):
        half = lax.rem(n, 2)
        slot = 2 + half
        slope_in(n, half).wait()

        @pl.when(n < TILES - 1)
        def _():
            slope_in(n + 1, 1 - half).start()

        @pl.when(n >= 2)
        def _():
            emit_copy(0, n - 2, slot).wait()

        for rc in range(BLOCKS):
            rows = slice(BLOCK * rc, BLOCK * rc + BLOCK)
            tile[rows] = (gp[4 * half + rc] * dot_t(g[rows], wd[0, tile_cols(n), :])).astype(BF16)
        emit(0, n, slot, dot(ut0[...], tile[...]))
        return 0

    lax.fori_loop(0, TILES, up_zero, 0)
    for n in (TILES - 2, TILES - 1):
        emit_copy(1, n, n % 2).wait()
        emit_copy(0, n, 2 + n % 2).wait()


def local_grads(x_rows, dh_rows, w_up, w_down, proj_up, proj_down):
    hbm = pl.BlockSpec(memory_space=pl.ANY)
    dma = pltpu.SemaphoreType.DMA
    return pl.pallas_call(
        grad_kernel,
        out_shape=(jax.ShapeDtypeStruct((4, 4, 4, 4, 2, 2, 8, 256), F32),
                   jax.ShapeDtypeStruct((TILES, BLOCKS, BLOCK, TILE), F32)),
        in_specs=[hbm] * 6,
        out_specs=(hbm, hbm),
        scratch_shapes=[
            pltpu.VMEM((2048, 768), BF16),
            pltpu.VMEM((2048, 768), BF16),
            pltpu.VMEM((2, 768, 2048), BF16),
            pltpu.VMEM((2, 2048, 768), BF16),
            pltpu.VMEM((2, 768, 256), BF16),
            pltpu.VMEM((2, 768, 256), BF16),
            pltpu.VMEM((2048, 2048), BF16),
            pltpu.VMEM((2048, 2048), BF16),
            pltpu.VMEM((256, 2048), BF16),
            pltpu.VMEM((256, 2048), BF16),
            pltpu.VMEM((256, 2048), BF16),
            pltpu.VMEM((TILES, BLOCK, TILE), F32),
            pltpu.VMEM((2048, TILE), BF16),
            pltpu.VMEM((4, 2, 4, 2, 2, 8, 256), F32),
            dma((8,)), dma((2,)), dma((4,)),
        ],
        compiler_params=pltpu.CompilerParams(vmem_limit_bytes=67_043_328),
    )(x_rows, dh_rows, w_up, w_down, proj_up, proj_down)


class Torus:
    def __init__(self):
        me = lax.axis_index("data")
        self.core = lax.rem(me, 2)
        chip = me // 2
        self.coords = (chip // 16, lax.rem(chip // 4, 4), lax.rem(chip, 4))
        self.partner = me + 1 - 2 * self.core

    def coord(self, axis, offset):
        return lax.rem(self.coords[axis] + offset, 4)

    def peer(self, axis, offset):
        z, y, x = (self.coord(a, offset) if a == axis else self.coords[a] for a in range(3))
        return ((z * 4 + y) * 4 + x) * 2 + self.core


def remote(src, dst, send_sem, recv_sem, device):
    return pltpu.make_async_remote_copy(
        src_ref=src, dst_ref=dst, send_sem=send_sem, recv_sem=recv_sem,
        device_id=(device,), device_id_type=MESH,
    )


def entry_barrier(torus):
    barrier = pltpu.get_barrier_semaphore()
    pl.semaphore_signal(barrier, inc=1, device_id=(torus.partner,), device_id_type=MESH)
    for axis in range(3):
        for offset in (1, 2, 3):
            pl.semaphore_signal(barrier, inc=1, device_id=(torus.peer(axis, offset),), device_id_type=MESH)
    pl.semaphore_wait(barrier, 10)


def at_axis(axes, axis, index):
    return tuple(index if a == axis else slice(None) for a in axes)


class Reducer:
    def __init__(self, torus, own, pair, rb1, part1, rb2, part2, rb3, red, gath, sems):
        self.torus = torus
        self.src = (own, part1, part2)
        self.got = (rb1, rb2, rb3)
        self.pair, self.red, self.gath = pair, red, gath
        self.rs_send, self.rs_recv, self.ag_send, self.ag_recv, self.swap_send, self.swap_recv = sems
        self.pending = []
        self.inbound = {}

    def add_pair(self, m):
        own, pair = self.src[0], self.pair

        def add_plane(z, _):
            own[m, z] = own[m, z] + pair[m, z]
            return 0

        lax.fori_loop(0, 4, add_plane, 0)

    def start(self, cp, key):
        cp.start()
        self.pending.append(cp)
        self.inbound.setdefault(key, []).append(cp)

    def arrive(self, key):
        for cp in self.inbound[key]:
            cp.wait_recv()

    def scatter(self, phase, m):
        for k, (half, lane, width) in enumerate(PIECES):
            order = ORDERS[COLOURS[m][k]]
            axis = order[phase]
            axes = tuple(a for a in range(3) if a not in order[:phase])
            tail = (half, slice(None), pl.ds(lane, width))
            for offset in (1, 2, 3):
                where = at_axis(axes, axis, self.torus.coord(axis, offset))
                rest = (slice(None),) * (len(axes) - 1)
                self.start(remote(
                    self.src[phase].at[(m,) + where + tail], self.got[phase].at[(m, offset - 1) + rest + tail],
                    self.rs_send.at[phase, m, k, offset - 1], self.rs_recv.at[phase, m, k, offset - 1],
                    self.torus.peer(axis, offset)), ("rs", phase, m, k))

    def collect(self, phase, m):
        for k, (half, lane, width) in enumerate(PIECES):
            order = ORDERS[COLOURS[m][k]]
            axis = order[phase]
            axes = tuple(a for a in range(3) if a not in order[:phase])
            tail = (half, slice(None), slice(lane, lane + width))
            rest = (slice(None),) * (len(axes) - 1)
            self.arrive(("rs", phase, m, k))
            got = self.got[phase]
            total = self.src[phase][(m,) + at_axis(axes, axis, self.torus.coords[axis]) + tail]
            for other in range(3):
                total = total + got[(m, other) + rest + tail]
            if phase < 2:
                self.src[phase + 1][(m,) + rest + tail] = total
            else:
                self.red[m, 8 * half:8 * half + 8, lane:lane + width] = total

    def update(self, m, moment, variance):
        z, y, x = self.torus.coords
        new_mom, new_var, direction = adam_shard(moment, variance, self.red[m])
        self.gath[m, z, y, x, self.torus.core] = direction
        return new_mom, new_var

    def spread(self, phase, m):
        for j in range(2):
            order = ORDERS[UNITS[m][j]][::-1]
            axis = order[phase]
            where = tuple(slice(None) if a in order[:phase] else self.torus.coords[a] for a in range(3))
            ref = self.gath.at[(m,) + where + (self.torus.core, slice(None), pl.ds(128 * j, 128))]
            for offset in (1, 2, 3):
                self.start(remote(
                    ref, ref, self.ag_send.at[phase, m, j, offset - 1], self.ag_recv.at[phase, m, j, offset - 1],
                    self.torus.peer(axis, offset)), ("ag", phase, m))

    def spread_arrive(self, phase, m):
        self.arrive(("ag", phase, m))

    def swap(self, m):
        ref = self.gath.at[m, :, :, :, self.torus.core]
        self.start(remote(ref, ref, self.swap_send.at[m], self.swap_recv.at[m], self.torus.partner), ("swap", m))

    def finish(self):
        for cp in self.pending:
            cp.wait_send()


def update_kernel(r_hbm, mom_up, var_up, mom_down, var_down, dir_out, mom_up_out, var_up_out, mom_down_out,
                  var_down_out, own, pair, rb1, part1, rb2, part2, rb3, red, gath, load_sem, pair_send, pair_recv,
                  rs_send, rs_recv, ag_send, ag_recv, swap_send, swap_recv, out_sem):
    torus = Torus()
    net = Reducer(torus, own, pair, rb1, part1, rb2, part2, rb3, red, gath,
                  (rs_send, rs_recv, ag_send, ag_recv, swap_send, swap_recv))
    order = (3, 2, 1, 0)
    loads = {}
    for m in order:
        loads[m] = pltpu.make_async_copy(r_hbm.at[m, :, :, :, torus.core], own.at[m], load_sem.at[m])
        loads[m].start()
    entry_barrier(torus)
    for m in order:
        net.start(remote(r_hbm.at[m, :, :, :, 1 - torus.core], pair.at[m], pair_send.at[m], pair_recv.at[m],
                         torus.partner), ("pair", m))
    for m in order:
        loads[m].wait()
        net.arrive(("pair", m))
        net.add_pair(m)
        net.scatter(0, m)
    for phase in (0, 1):
        for m in order:
            net.collect(phase, m)
            net.scatter(phase + 1, m)
    state = ((mom_up, var_up, mom_up_out, var_up_out), (mom_down, var_down, mom_down_out, var_down_out))
    for m in order:
        net.collect(2, m)
        mom, var, mom_out, var_out = state[m % 2]
        mom_out[m // 2], var_out[m // 2] = net.update(m, mom[m // 2], var[m // 2])
        net.spread(0, m)
    for phase in (0, 1):
        for m in order:
            net.spread_arrive(phase, m)
            net.spread(phase + 1, m)
    for m in order:
        net.spread_arrive(2, m)
        net.swap(m)
    outs = []
    for m in order:
        net.arrive(("swap", m))
        cp = pltpu.make_async_copy(gath.at[m], dir_out.at[m], out_sem.at[m])
        cp.start()
        outs.append(cp)
    net.finish()
    for cp in outs:
        cp.wait()


def reduce_update(parts, moments):
    dma = pltpu.SemaphoreType.DMA
    hbm = pl.BlockSpec(memory_space=pl.ANY)
    vmem = pl.BlockSpec(memory_space=pltpu.VMEM)
    shard = jax.ShapeDtypeStruct((2, 16, 256), F32)
    return pl.pallas_call(
        update_kernel,
        out_shape=(jax.ShapeDtypeStruct((4, 4, 4, 4, 2, 16, 256), BF16),) + (shard,) * 4,
        in_specs=[hbm] + [vmem] * 4,
        out_specs=(hbm,) + (vmem,) * 4,
        scratch_shapes=[
            pltpu.VMEM((4, 4, 4, 4, 2, 8, 256), F32),
            pltpu.VMEM((4, 4, 4, 4, 2, 8, 256), F32),
            pltpu.VMEM((4, 3, 4, 4, 2, 8, 256), F32),
            pltpu.VMEM((4, 4, 4, 2, 8, 256), F32),
            pltpu.VMEM((4, 3, 4, 2, 8, 256), F32),
            pltpu.VMEM((4, 4, 2, 8, 256), F32),
            pltpu.VMEM((4, 3, 2, 8, 256), F32),
            pltpu.VMEM((4, 16, 256), F32),
            pltpu.VMEM((4, 4, 4, 4, 2, 16, 256), BF16),
            dma((4,)), dma((4,)), dma((4,)),
            dma((3, 4, 3, 3)), dma((3, 4, 3, 3)),
            dma((3, 4, 2, 3)), dma((3, 4, 2, 3)),
            dma((4,)), dma((4,)), dma((4,)),
        ],
        compiler_params=pltpu.CompilerParams(collective_id=0, has_side_effects=True),
    )(parts, *moments)


def weight_kernel(dir_up, dir_down, w_up, w_down, proj_up, proj_down, new_up, new_down):
    new_up[0] = (w_up[0] - SCALE * dot_t(proj_up[0], dir_up[0])).astype(BF16)
    new_down[0] = (w_down[0] - SCALE * dot_t(dir_down[0], proj_down[0])).astype(BF16)


def new_weights(directions, w_up, w_down, proj_up, proj_down):
    width = 512
    up_spec = pl.BlockSpec((1, 768, width), lambda l, n: (l, 0, n))
    down_spec = pl.BlockSpec((1, width, 768), lambda l, n: (l, n, 0))
    proj_spec = pl.BlockSpec((1, 768, 256), lambda l, n: (l, 0, 0))
    return pl.pallas_call(
        weight_kernel,
        grid=(2, 2048 // width),
        out_shape=(jax.ShapeDtypeStruct(w_up.shape, BF16), jax.ShapeDtypeStruct(w_down.shape, BF16)),
        in_specs=[
            pl.BlockSpec((1, width, 256), lambda l, n: (2 * l, n, 0)),
            pl.BlockSpec((1, width, 256), lambda l, n: (2 * l + 1, n, 0)),
            up_spec, down_spec, proj_spec, proj_spec,
        ],
        out_specs=(up_spec, down_spec),
    )(directions, directions, w_up, w_down, proj_up, proj_down)


def solution(mesh):
    def local_step(x_loc, dh_loc, w_up, w_down, proj_up, proj_down, mom_up, var_up, mom_down, var_down):
        parts, _ = local_grads(x_loc, dh_loc, w_up, w_down, proj_up, proj_down)
        moments = (jnp.swapaxes(mom_up, 1, 2), jnp.swapaxes(var_up, 1, 2), mom_down, var_down)
        directions, *moments = reduce_update(parts, moments)
        weights = new_weights(directions.reshape(4, 2048, 256), w_up, w_down, proj_up, proj_down)
        return (*weights, jnp.swapaxes(moments[0], 1, 2), jnp.swapaxes(moments[1], 1, 2), moments[2], moments[3])

    tok_spec = P('data', None)
    up_spec = P(None, None, 'data')
    down_spec = P(None, 'data', None)
    return jax.shard_map(
        local_step,
        mesh=mesh,
        in_specs=(tok_spec, tok_spec, P(), P(), P(), P(), up_spec, up_spec, down_spec, down_spec),
        out_specs=(P(), P(), up_spec, up_spec, down_spec, down_spec),
        check_vma=False,
    )
```

```python
import jax
import jax.numpy as jnp
from jax import lax
from jax.experimental import pallas as pl
from jax.experimental.pallas import tpu as pltpu
from jax.sharding import PartitionSpec as P

BETA_ONE = 0.9
BETA_TWO = 0.999
EPSILON = 1e-8
STEP = 4
LEARN_RATE = 0.02
ALPHA_SCALE = 0.25
SCALE = LEARN_RATE * ALPHA_SCALE
GELU_A = 0.7978845608028654
GELU_B = 0.044715
MESH = pl.DeviceIdType.MESH
F32, BF16 = jnp.float32, jnp.bfloat16

BLOCK = 512
TILE = 256
BLOCKS = 4
TILES = 8

ORDERS = ((2, 1, 0), (1, 0, 2), (0, 2, 1))
COLOURS = ((0, 1, 2), (1, 2, 0), (2, 0, 1), (0, 1, 2))
PIECES = ((0, 0, 256), (1, 0, 128), (1, 128, 128))
UNITS = ((0, 1), (2, 0), (1, 2), (0, 1))


def dot(lhs, rhs):
    return jnp.dot(lhs, rhs, preferred_element_type=F32)


def dot_t(lhs, rhs):
    return lax.dot_general(lhs, rhs, (((1,), (1,)), ((), ())), preferred_element_type=F32)


def gelu_pair(z):
    sq = z * z
    cdf = 0.5 + 0.5 * jnp.tanh(z * (GELU_A + (GELU_A * GELU_B) * sq))
    act = z * cdf
    slope = cdf + act * ((1.0 - cdf) * (2.0 * GELU_A + (6.0 * GELU_A * GELU_B) * sq))
    return act, slope


def adam_shard(moment, variance, grad_red):
    new_mom = BETA_ONE * moment + (1.0 - BETA_ONE) * grad_red
    new_var = BETA_TWO * variance + (1.0 - BETA_TWO) * grad_red * grad_red
    bias_one = 1.0 - BETA_ONE ** STEP
    bias_two = 1.0 - BETA_TWO ** STEP
    direction = (new_mom / bias_one) / (jnp.sqrt(new_var / bias_two) + EPSILON)
    return new_mom, new_var, direction.astype(BF16)


def block_rows(i):
    return pl.ds(pl.multiple_of(i * BLOCK, BLOCK), BLOCK)


def tile_cols(n):
    return pl.ds(pl.multiple_of(n * TILE, TILE), TILE)


class Torus:
    def __init__(self):
        me = lax.axis_index("data")
        self.core = lax.rem(me, 2)
        chip = me // 2
        self.coords = (chip // 16, lax.rem(chip // 4, 4), lax.rem(chip, 4))
        self.partner = me + 1 - 2 * self.core

    def coord(self, axis, offset):
        return lax.rem(self.coords[axis] + offset, 4)

    def peer(self, axis, offset):
        z, y, x = (self.coord(a, offset) if a == axis else self.coords[a] for a in range(3))
        return ((z * 4 + y) * 4 + x) * 2 + self.core


def remote(src, dst, send_sem, recv_sem, device):
    return pltpu.make_async_remote_copy(
        src_ref=src, dst_ref=dst, send_sem=send_sem, recv_sem=recv_sem,
        device_id=(device,), device_id_type=MESH,
    )


def entry_barrier(torus):
    barrier = pltpu.get_barrier_semaphore()
    pl.semaphore_signal(barrier, inc=1, device_id=(torus.partner,), device_id_type=MESH)
    for axis in range(3):
        for offset in (1, 2, 3):
            pl.semaphore_signal(barrier, inc=1, device_id=(torus.peer(axis, offset),), device_id_type=MESH)
    return lambda: pl.semaphore_wait(barrier, 10)


def at_axis(axes, axis, index):
    return tuple(index if a == axis else slice(None) for a in axes)


class Reducer:
    def __init__(self, torus, tiles, own, pair, rb1, part1, rb2, part2, rb3, red, gath, sems):
        self.torus = torus
        self.tiles = tiles
        self.src = (own, part1, part2)
        self.got = (rb1, rb2, rb3)
        self.pair, self.red, self.gath = pair, red, gath
        (self.pair_send, self.pair_recv, self.rs_send, self.rs_recv, self.ag_send, self.ag_recv, self.swap_send,
         self.swap_recv) = sems
        self.pending = []
        self.inbound = {}

    def pair_copy(self, m, n, slot):
        where = (m, n // 2, pl.ds(2 * lax.rem(n, 2), 2))
        return remote(self.tiles.at[slot, :, :, 1 - self.torus.core], self.pair.at[where],
                      self.pair_send.at[slot], self.pair_recv.at[m, n], self.torus.partner)

    def emit(self, m, n, slot, part):
        self.tiles[slot] = part.T.reshape(2, 4, 2, 2, 8, 256)
        self.src[0][m, n // 2, pl.ds(2 * lax.rem(n, 2), 2)] = self.tiles[slot, :, :, self.torus.core]
        self.pair_copy(m, n, slot).start()

    def begin(self, m):
        for n in range(TILES):
            self.pair_copy(m, n, 0).wait_recv()
        self.add_pair(m)
        self.scatter(0, m)

    def step(self, phase, m):
        self.collect(phase, m)
        self.scatter(phase + 1, m)

    def pass_on(self, phase, m):
        self.spread_arrive(phase, m)
        self.spread(phase + 1, m)

    def add_pair(self, m):
        own, pair = self.src[0], self.pair

        def add_plane(z, _):
            own[m, z] = own[m, z] + pair[m, z]
            return 0

        lax.fori_loop(0, 4, add_plane, 0)

    def start(self, cp, key):
        cp.start()
        self.pending.append(cp)
        self.inbound.setdefault(key, []).append(cp)

    def arrive(self, key):
        for cp in self.inbound[key]:
            cp.wait_recv()

    def scatter(self, phase, m):
        for k, (half, lane, width) in enumerate(PIECES):
            order = ORDERS[COLOURS[m][k]]
            axis = order[phase]
            axes = tuple(a for a in range(3) if a not in order[:phase])
            tail = (half, slice(None), pl.ds(lane, width))
            for offset in (1, 2, 3):
                where = at_axis(axes, axis, self.torus.coord(axis, offset))
                rest = (slice(None),) * (len(axes) - 1)
                self.start(remote(
                    self.src[phase].at[(m,) + where + tail], self.got[phase].at[(m, offset - 1) + rest + tail],
                    self.rs_send.at[phase, m, k, offset - 1], self.rs_recv.at[phase, m, k, offset - 1],
                    self.torus.peer(axis, offset)), ("rs", phase, m, k))

    def collect(self, phase, m):
        for k, (half, lane, width) in enumerate(PIECES):
            order = ORDERS[COLOURS[m][k]]
            axis = order[phase]
            axes = tuple(a for a in range(3) if a not in order[:phase])
            tail = (half, slice(None), slice(lane, lane + width))
            rest = (slice(None),) * (len(axes) - 1)
            self.arrive(("rs", phase, m, k))
            got = self.got[phase]
            total = self.src[phase][(m,) + at_axis(axes, axis, self.torus.coords[axis]) + tail]
            for other in range(3):
                total = total + got[(m, other) + rest + tail]
            if phase < 2:
                self.src[phase + 1][(m,) + rest + tail] = total
            else:
                self.red[m, 8 * half:8 * half + 8, lane:lane + width] = total

    def update(self, m, moment, variance):
        z, y, x = self.torus.coords
        new_mom, new_var, direction = adam_shard(moment, variance, self.red[m])
        self.gath[m, z, y, x, self.torus.core] = direction
        return new_mom, new_var

    def spread(self, phase, m):
        for j in range(2):
            order = ORDERS[UNITS[m][j]][::-1]
            axis = order[phase]
            where = tuple(slice(None) if a in order[:phase] else self.torus.coords[a] for a in range(3))
            ref = self.gath.at[(m,) + where + (self.torus.core, slice(None), pl.ds(128 * j, 128))]
            for offset in (1, 2, 3):
                self.start(remote(
                    ref, ref, self.ag_send.at[phase, m, j, offset - 1], self.ag_recv.at[phase, m, j, offset - 1],
                    self.torus.peer(axis, offset)), ("ag", phase, m))

    def spread_arrive(self, phase, m):
        self.arrive(("ag", phase, m))

    def swap(self, m):
        self.spread_arrive(2, m)
        ref = self.gath.at[m, :, :, :, self.torus.core]
        self.start(remote(ref, ref, self.swap_send.at[m], self.swap_recv.at[m], self.torus.partner), ("swap", m))

    def finish(self):
        for cp in self.pending:
            cp.wait_send()


def step_kernel(x_hbm, dh_hbm, wu_hbm, wd_hbm, pu_hbm, pd_hbm, mom_up, var_up, mom_down, var_down,
                dir_out, mom_up_out, var_up_out, mom_down_out, var_down_out, gp_hbm,
                h, g, wu, wd, pu, pd, act, dz, ut0, gp, tile, tiles,
                own, pair, rb1, part1, rb2, part2, rb3, red, gath,
                in_sem, gp_sem, out_sem, pair_send, pair_recv, rs_send, rs_recv, ag_send, ag_recv,
                swap_send, swap_recv):
    torus = Torus()
    net = Reducer(torus, tiles, own, pair, rb1, part1, rb2, part2, rb3, red, gath,
                  (pair_send, pair_recv, rs_send, rs_recv, ag_send, ag_recv, swap_send, swap_recv))
    state = ((mom_up, var_up, mom_up_out, var_up_out), (mom_down, var_down, mom_down_out, var_down_out))

    def update(m):
        net.collect(2, m)
        mom, var, mom_out, var_out = state[m % 2]
        mom_out[m // 2], var_out[m // 2] = net.update(m, mom[m // 2], var[m // 2])
        net.spread(0, m)

    ut1, vt = wu.at[0, 0:256], wu.at[0, 256:512]
    loads = {}

    def load(name, src, dst):
        cp = pltpu.make_async_copy(src, dst, in_sem.at[len(loads)])
        cp.start()
        loads[name] = cp

    load("x", x_hbm, h)
    load("wu0", wu_hbm.at[0], wu.at[0])
    load("pu", pu_hbm, pu)
    load("wd0", wd_hbm.at[0], wd.at[0])
    load("dh", dh_hbm, g)
    load("pd", pd_hbm, pd)
    load("wu1", wu_hbm.at[1], wu.at[1])
    load("wd1", wd_hbm.at[1], wd.at[1])
    peers_ready = entry_barrier(torus)

    def slope_out(rb):
        return pltpu.make_async_copy(own, gp_hbm.at[rb], gp_sem.at[0])

    def slope_in(n, rc):
        return pltpu.make_async_copy(
            gp_hbm.at[rc, n // 2, pl.ds(2 * lax.rem(n, 2), 2)], gp.at[rc], gp_sem.at[rc])

    for name in ("x", "wu0", "pu", "wd0"):
        loads[name].wait()

    def forward_zero(rb, _):
        rows = block_rows(rb)
        ut0[:, rows] = dot(h[rows], pu[0]).astype(BF16).T
        for n in range(TILES):
            cols = slice(TILE * n, TILE * n + TILE)
            value, slope = gelu_pair(dot(h[rows], wu[0, :, cols]))
            act[rows, cols] = value.astype(BF16)
            own[n // 2, 2 * (n % 2):2 * (n % 2) + 2] = slope.reshape(2, 4, 4, 2, 8, 256)
        cp = slope_out(rb)
        cp.start()
        for k in range(3):
            cols = slice(256 * k, 256 * k + 256)
            h[rows, cols] = (h[rows, cols] + dot(act[rows], wd[0, :, cols])).astype(BF16)
        cp.wait()
        return 0

    lax.fori_loop(0, BLOCKS, forward_zero, 0)
    for name in ("dh", "pd", "wu1", "wd1"):
        loads[name].wait()
    peers_ready()

    def project_one(rb, _):
        rows = block_rows(rb)
        ut1[:, rows] = dot(h[rows], pu[1]).astype(BF16).T
        vt[:, rows] = dot(g[rows], pd[1]).astype(BF16).T
        return 0

    lax.fori_loop(0, BLOCKS, project_one, 0)

    def layer_one(n, _):
        cols = tile_cols(n)
        slot = 2 * lax.rem(n, 2)

        @pl.when(n >= 2)
        def _():
            net.pair_copy(3, n - 2, slot).wait_send()
            net.pair_copy(2, n - 2, slot + 1).wait_send()

        for rc in range(BLOCKS):
            rows = slice(BLOCK * rc, BLOCK * rc + BLOCK)
            value, slope = gelu_pair(dot(h[rows], wu[1, :, cols]))
            tile[rows] = value.astype(BF16)
            dz[rows, cols] = (slope * dot_t(g[rows], wd[1, cols, :])).astype(BF16)
        net.emit(3, n, slot, dot(vt[...], tile[...]))
        net.emit(2, n, slot + 1, dot(ut1[...], dz[:, cols]))
        return 0

    lax.fori_loop(0, TILES, layer_one, 0)

    def input_grad(rb, _):
        rows = block_rows(rb)
        for k in range(3):
            cols = slice(256 * k, 256 * k + 256)
            g[rows, cols] = (g[rows, cols] + dot_t(dz[rows], wu[1, cols, :])).astype(BF16)
        vt[:, rows] = dot(g[rows], pd[0]).astype(BF16).T
        return 0

    lax.fori_loop(0, 1, input_grad, 0)
    net.begin(3)
    net.begin(2)
    lax.fori_loop(1, BLOCKS, input_grad, 0)
    for n in (TILES - 2, TILES - 1):
        net.pair_copy(3, n, 2 * (n % 2)).wait_send()
        net.pair_copy(2, n, 2 * (n % 2) + 1).wait_send()

    def down_zero(n, _):
        slot = lax.rem(n, 2)

        @pl.when(n >= 2)
        def _():
            net.pair_copy(1, n - 2, slot).wait_send()

        net.emit(1, n, slot, dot(vt[...], act[:, tile_cols(n)]))
        return 0

    for rc in range(BLOCKS):
        slope_in(0, rc).start()
    lax.fori_loop(0, TILES, down_zero, 0)

    def up_zero(n, _):
        slot = 2 + lax.rem(n, 2)
        after = lax.min(n + 1, TILES - 1)

        @pl.when(n >= 2)
        def _():
            net.pair_copy(0, n - 2, slot).wait_send()

        for rc in range(BLOCKS):
            rows = slice(BLOCK * rc, BLOCK * rc + BLOCK)
            slope_in(n, rc).wait()
            d_act = dot_t(g[rows], wd[0, tile_cols(n), :])
            tile[rows] = (gp[rc].reshape(BLOCK, TILE) * d_act).astype(BF16)
            if rc:
                slope_in(after, rc - 1).start()
        slope_in(after, BLOCKS - 1).start()
        net.emit(0, n, slot, dot(ut0[...], tile[...]))
        return 0

    lax.fori_loop(0, 1, up_zero, 0)
    net.begin(1)
    lax.fori_loop(1, 3, up_zero, 0)
    net.step(0, 3)
    net.step(0, 2)
    lax.fori_loop(3, 5, up_zero, 0)
    net.step(1, 3)
    net.step(1, 2)
    lax.fori_loop(5, 7, up_zero, 0)
    update(3)
    update(2)
    net.step(0, 1)
    lax.fori_loop(7, 8, up_zero, 0)
    for rc in range(BLOCKS):
        slope_in(TILES - 1, rc).wait()
    net.begin(0)
    net.pass_on(0, 3)
    net.pass_on(0, 2)
    net.step(1, 1)
    net.step(0, 0)
    net.pass_on(1, 3)
    net.pass_on(1, 2)
    update(1)
    net.step(1, 0)
    net.pass_on(0, 1)
    update(0)
    net.swap(3)
    net.swap(2)
    net.pass_on(1, 1)
    net.pass_on(0, 0)
    outs = []

    def result(m):
        net.arrive(("swap", m))
        cp = pltpu.make_async_copy(gath.at[m], dir_out.at[m], out_sem.at[m])
        cp.start()
        outs.append(cp)

    result(3)
    result(2)
    net.pass_on(1, 0)
    net.swap(1)
    net.swap(0)
    result(1)
    result(0)
    for n in (TILES - 2, TILES - 1):
        net.pair_copy(1, n, n % 2).wait_send()
        net.pair_copy(0, n, 2 + n % 2).wait_send()
    net.finish()
    for cp in outs:
        cp.wait()


def train_step(x_rows, dh_rows, w_up, w_down, proj_up, proj_down, moments):
    hbm = pl.BlockSpec(memory_space=pl.ANY)
    vmem = pl.BlockSpec(memory_space=pltpu.VMEM)
    dma = pltpu.SemaphoreType.DMA
    shard = jax.ShapeDtypeStruct((2, 16, 256), F32)
    return pl.pallas_call(
        step_kernel,
        out_shape=(jax.ShapeDtypeStruct((4, 4, 4, 4, 2, 16, 256), BF16),) + (shard,) * 4
        + (jax.ShapeDtypeStruct((BLOCKS, 4, 4, 4, 4, 2, 8, 256), F32),),
        in_specs=[hbm] * 6 + [vmem] * 4,
        out_specs=(hbm,) + (vmem,) * 4 + (hbm,),
        scratch_shapes=[
            pltpu.VMEM((2048, 768), BF16),
            pltpu.VMEM((2048, 768), BF16),
            pltpu.VMEM((2, 768, 2048), BF16),
            pltpu.VMEM((2, 2048, 768), BF16),
            pltpu.VMEM((2, 768, 256), BF16),
            pltpu.VMEM((2, 768, 256), BF16),
            pltpu.VMEM((2048, 2048), BF16),
            pltpu.VMEM((2048, 2048), BF16),
            pltpu.VMEM((256, 2048), BF16),
            pltpu.VMEM((BLOCKS, 2, 4, 4, 2, 8, 256), F32),
            pltpu.VMEM((2048, TILE), BF16),
            pltpu.VMEM((4, 2, 4, 2, 2, 8, 256), F32),
            pltpu.VMEM((4, 4, 4, 4, 2, 8, 256), F32),
            pltpu.VMEM((4, 4, 4, 4, 2, 8, 256), F32),
            pltpu.VMEM((4, 3, 4, 4, 2, 8, 256), F32),
            pltpu.VMEM((4, 4, 4, 2, 8, 256), F32),
            pltpu.VMEM((4, 3, 4, 2, 8, 256), F32),
            pltpu.VMEM((4, 4, 2, 8, 256), F32),
            pltpu.VMEM((4, 3, 2, 8, 256), F32),
            pltpu.VMEM((4, 16, 256), F32),
            pltpu.VMEM((4, 4, 4, 4, 2, 16, 256), BF16),
            dma((8,)), dma((BLOCKS,)), dma((4,)), dma((4,)), dma((4, TILES)),
            dma((3, 4, 3, 3)), dma((3, 4, 3, 3)),
            dma((3, 4, 2, 3)), dma((3, 4, 2, 3)),
            dma((4,)), dma((4,)),
        ],
        compiler_params=pltpu.CompilerParams(
            collective_id=0, has_side_effects=True, vmem_limit_bytes=67_043_328),
    )(x_rows, dh_rows, w_up, w_down, proj_up, proj_down, *moments)


def weight_kernel(dir_up, dir_down, w_up, w_down, proj_up, proj_down, *refs):
    moments, new_up, new_down, outs = refs[:4], refs[4], refs[5], refs[6:]

    @pl.when((pl.program_id(0) == 0) & (pl.program_id(1) == 0))
    def _():
        for src, dst in zip(moments, outs):
            dst[...] = src[...]

    new_up[0] = (w_up[0] - SCALE * dot_t(proj_up[0], dir_up[0])).astype(BF16)
    new_down[0] = (w_down[0] - SCALE * dot_t(dir_down[0], proj_down[0])).astype(BF16)


def new_weights(directions, w_up, w_down, proj_up, proj_down, moments):
    width = 512
    up_spec = pl.BlockSpec((1, 768, width), lambda l, n: (l, 0, n))
    down_spec = pl.BlockSpec((1, width, 768), lambda l, n: (l, n, 0))
    proj_spec = pl.BlockSpec((1, 768, 256), lambda l, n: (l, 0, 0))
    shard_spec = pl.BlockSpec((2, 16, 256), lambda l, n: (0, 0, 0))
    return pl.pallas_call(
        weight_kernel,
        grid=(2, 2048 // width),
        out_shape=(jax.ShapeDtypeStruct(w_up.shape, BF16), jax.ShapeDtypeStruct(w_down.shape, BF16))
        + (jax.ShapeDtypeStruct((2, 16, 256), F32),) * 4,
        in_specs=[
            pl.BlockSpec((1, width, 256), lambda l, n: (2 * l, n, 0)),
            pl.BlockSpec((1, width, 256), lambda l, n: (2 * l + 1, n, 0)),
            up_spec, down_spec, proj_spec, proj_spec,
        ] + [shard_spec] * 4,
        out_specs=(up_spec, down_spec) + (shard_spec,) * 4,
    )(directions, directions, w_up, w_down, proj_up, proj_down, *moments)


def solution(mesh):
    def local_step(x_loc, dh_loc, w_up, w_down, proj_up, proj_down, mom_up, var_up, mom_down, var_down):
        moments = (jnp.swapaxes(mom_up, 1, 2), jnp.swapaxes(var_up, 1, 2), mom_down, var_down)
        directions, *moments, _ = train_step(x_loc, dh_loc, w_up, w_down, proj_up, proj_down, moments)
        new_up, new_down, *moments = new_weights(
            directions.reshape(4, 2048, 256), w_up, w_down, proj_up, proj_down, moments)
        return (new_up, new_down, jnp.swapaxes(moments[0], 1, 2), jnp.swapaxes(moments[1], 1, 2), moments[2], moments[3])

    tok_spec = P('data', None)
    up_spec = P(None, None, 'data')
    down_spec = P(None, 'data', None)
    return jax.shard_map(
        local_step,
        mesh=mesh,
        in_specs=(tok_spec, tok_spec, P(), P(), P(), P(), up_spec, up_spec, down_spec, down_spec),
        out_specs=(P(), P(), up_spec, up_spec, down_spec, down_spec),
        check_vma=False,
    )
```

```python
import jax
import jax.numpy as jnp
from jax import lax
from jax.experimental import pallas as pl
from jax.experimental.pallas import tpu as pltpu
from jax.sharding import PartitionSpec as P

BETA_ONE = 0.9
BETA_TWO = 0.999
EPSILON = 1e-8
STEP = 4
LEARN_RATE = 0.02
ALPHA_SCALE = 0.25
SCALE = LEARN_RATE * ALPHA_SCALE
GELU_A = 0.7978845608028654
GELU_B = 0.044715
MESH = pl.DeviceIdType.MESH
ALL = slice(None)
ROWS, WIDTH, FF, RANK = 2048, 768, 2048, 256
F32, BF16 = jnp.float32, jnp.bfloat16

PIECE = (2, 4, 4, 2, 8, RANK)
DIRECTIONS = (4,) * 4 + (2, 16, RANK)
BLOCK = 512
TILE = 256
BLOCKS = 4
TILES = 8

ORDERS = ((2, 1, 0), (1, 0, 2), (0, 2, 1))
COLOURS = ((0, 1, 2), (1, 2, 0), (2, 0, 1), (0, 1, 2))
PIECES = ((0, 0, 256), (1, 0, 128), (1, 128, 128))
UNITS = ((0, 1), (2, 0), (1, 2), (0, 1))
SCHEDULE = (
    (2, "all1 line3 line2"),
    (4, "plane3 plane2"),
    (6, "adam3 adam2 line1"),
    (8, "pass3 pass2 plane1"),
)
LAST = ("begin0",)
TAIL = (
    "fan3 fan2 adam1 line0", "plane0 pass1", "adam0 swap3 swap2",
    "fan1 pass0 out3 out2", "fan0 swap1 swap0",
)


def dot(lhs, rhs):
    return jnp.dot(lhs, rhs, preferred_element_type=F32)


def dot_t(lhs, rhs):
    return lax.dot_general(lhs, rhs, (((1,), (1,)), ((), ())), preferred_element_type=F32)


def gelu_pair(z):
    sq = z * z
    cdf = 0.5 + 0.5 * jnp.tanh(z * (GELU_A + (GELU_A * GELU_B) * sq))
    act = z * cdf
    slope = cdf + act * ((1.0 - cdf) * (2.0 * GELU_A + (6.0 * GELU_A * GELU_B) * sq))
    return act, slope


def adam_shard(moment, variance, grad_red):
    new_mom = BETA_ONE * moment + (1.0 - BETA_ONE) * grad_red
    new_var = BETA_TWO * variance + (1.0 - BETA_TWO) * grad_red * grad_red
    bias_one = 1.0 - BETA_ONE ** STEP
    bias_two = 1.0 - BETA_TWO ** STEP
    direction = (new_mom / bias_one) / (jnp.sqrt(new_var / bias_two) + EPSILON)
    return new_mom, new_var, direction.astype(BF16)


def block_rows(i):
    return pl.ds(pl.multiple_of(i * BLOCK, BLOCK), BLOCK)


def tile_cols(n):
    return pl.ds(pl.multiple_of(n * TILE, TILE), TILE)


class Torus:
    def __init__(self):
        me = lax.axis_index("data")
        self.core = lax.rem(me, 2)
        chip = me // 2
        self.coords = (chip // 16, lax.rem(chip // 4, 4), lax.rem(chip, 4))
        self.partner = me + 1 - 2 * self.core

    def coord(self, axis, offset):
        return lax.rem(self.coords[axis] + offset, 4)

    def peer(self, axis, offset):
        z, y, x = (self.coord(a, offset) if a == axis else self.coords[a] for a in range(3))
        return ((z * 4 + y) * 4 + x) * 2 + self.core


def remote(src, dst, send_sem, recv_sem, device):
    return pltpu.make_async_remote_copy(
        src_ref=src, dst_ref=dst, send_sem=send_sem, recv_sem=recv_sem,
        device_id=(device,), device_id_type=MESH,
    )


def entry_barrier(torus):
    barrier = pltpu.get_barrier_semaphore()
    pl.semaphore_signal(barrier, inc=1, device_id=(torus.partner,), device_id_type=MESH)
    for axis in range(3):
        for offset in (1, 2, 3):
            pl.semaphore_signal(barrier, inc=1, device_id=(torus.peer(axis, offset),), device_id_type=MESH)
    return lambda: pl.semaphore_wait(barrier, 10)


def at_axis(axes, axis, index):
    return tuple(index if a == axis else ALL for a in axes)


class Reducer:
    def __init__(self, torus, tiles, own, pair, rb1, part1, rb2, part2, rb3, red, gath, sems):
        self.torus = torus
        self.tiles = tiles
        self.src = (own, part1, part2)
        self.got = (rb1, rb2, rb3)
        self.pair, self.red, self.gath = pair, red, gath
        (self.pair_send, self.pair_recv, self.rs_send, self.rs_recv, self.ag_send, self.ag_recv, self.swap_send,
         self.swap_recv) = sems
        self.pending = []
        self.inbound = {}

    def pair_copy(self, m, n, slot):
        where = (m, n // 2, pl.ds(2 * lax.rem(n, 2), 2))
        return remote(self.tiles.at[slot, :, :, 1 - self.torus.core], self.pair.at[where],
                      self.pair_send.at[slot], self.pair_recv.at[m, n], self.torus.partner)

    def emit(self, m, n, slot, part):
        self.tiles[slot] = part.T.reshape(2, 4, 2, 2, 8, 256)
        self.src[0][m, n // 2, pl.ds(2 * lax.rem(n, 2), 2)] = self.tiles[slot, :, :, self.torus.core]
        self.pair_copy(m, n, slot).start()

    def slab(self, m, z):
        own, pair = self.src[0], self.pair
        for half in range(2):
            self.pair_copy(m, 2 * z + half, 0).wait_recv()
        own[m, z] = own[m, z] + pair[m, z]
        for k, (half, lane, width) in enumerate(PIECES):
            axis = ORDERS[COLOURS[m][k]][0]
            tail = (half, ALL, pl.ds(lane, width))
            if axis == 0:
                offset = lax.rem(z + 4 - self.torus.coords[0], 4)

                @pl.when(offset > 0)
                def _():
                    self.copy(own.at[(m, z) + (ALL,) * 2 + tail],
                              self.got[0].at[(m, offset - 1) + (ALL,) * 2 + tail],
                              (0, m, k, offset - 1), self.torus.peer(0, offset)).start()
                continue
            for offset in (1, 2, 3):
                where = at_axis((1, 2), axis, self.torus.coord(axis, offset))
                self.copy(own.at[(m, z) + where + tail], self.got[0].at[(m, offset - 1, z, ALL) + tail],
                          (0, m, k, offset - 1), self.torus.peer(axis, offset)).start()

    def begin(self, m):
        self.slab(m, 3)
        self.scatter(0, m, False)

    def begin_all(self, m):
        lax.fori_loop(0, 3, lambda z, _: (self.slab(m, z), 0)[1], 0)
        self.begin(m)

    def copy(self, src, dst, sem, device):
        return remote(src, dst, self.rs_send.at[sem], self.rs_recv.at[sem], device)

    def step(self, phase, m):
        self.collect(phase, m)
        self.scatter(phase + 1, m)

    def pass_on(self, phase, m):
        self.spread_arrive(phase, m)
        self.spread(phase + 1, m)

    def start(self, cp, key, go=True):
        if go:
            cp.start()
        self.pending.append(cp)
        self.inbound.setdefault(key, []).append(cp)

    def arrive(self, key):
        for cp in self.inbound[key]:
            cp.wait_recv()

    def scatter(self, phase, m, go=True):
        for k, (half, lane, width) in enumerate(PIECES):
            order = ORDERS[COLOURS[m][k]]
            axis = order[phase]
            axes = tuple(a for a in range(3) if a not in order[:phase])
            tail = (half, ALL, pl.ds(lane, width))
            for offset in (1, 2, 3):
                where = at_axis(axes, axis, self.torus.coord(axis, offset))
                rest = (ALL,) * (len(axes) - 1)
                self.start(self.copy(
                    self.src[phase].at[(m,) + where + tail], self.got[phase].at[(m, offset - 1) + rest + tail],
                    (phase, m, k, offset - 1), self.torus.peer(axis, offset)), ("rs", phase, m, k), go)

    def collect(self, phase, m):
        for k, (half, lane, width) in enumerate(PIECES):
            order = ORDERS[COLOURS[m][k]]
            axis = order[phase]
            axes = tuple(a for a in range(3) if a not in order[:phase])
            tail = (half, ALL, slice(lane, lane + width))
            rest = (ALL,) * (len(axes) - 1)
            self.arrive(("rs", phase, m, k))
            got = self.got[phase]
            total = self.src[phase][(m,) + at_axis(axes, axis, self.torus.coords[axis]) + tail]
            for other in range(3):
                total = total + got[(m, other) + rest + tail]
            if phase < 2:
                self.src[phase + 1][(m,) + rest + tail] = total
            else:
                self.red[m, 8 * half:8 * half + 8, lane:lane + width] = total

    def update(self, m, moment, variance):
        z, y, x = self.torus.coords
        new_mom, new_var, direction = adam_shard(moment, variance, self.red[m])
        self.gath[m, z, y, x, self.torus.core] = direction
        return new_mom, new_var

    def spread(self, phase, m):
        for j in range(2):
            order = ORDERS[UNITS[m][j]][::-1]
            axis = order[phase]
            where = tuple(ALL if a in order[:phase] else self.torus.coords[a] for a in range(3))
            ref = self.gath.at[(m,) + where + (self.torus.core, ALL, pl.ds(128 * j, 128))]
            for offset in (1, 2, 3):
                self.start(remote(
                    ref, ref, self.ag_send.at[phase, m, j, offset - 1], self.ag_recv.at[phase, m, j, offset - 1],
                    self.torus.peer(axis, offset)), ("ag", phase, m))

    def spread_arrive(self, phase, m):
        self.arrive(("ag", phase, m))

    def swap(self, m):
        self.spread_arrive(2, m)
        ref = self.gath.at[m, :, :, :, self.torus.core]
        self.start(remote(ref, ref, self.swap_send.at[m], self.swap_recv.at[m], self.torus.partner), ("swap", m))

    def finish(self):
        for cp in self.pending:
            cp.wait_send()
        self.pending = []


def step_kernel(x_hbm, dh_hbm, wu_hbm, wd_hbm, pu_hbm, pd_hbm, mom_up, var_up, mom_down, var_down,
                dir_out, mom_up_out, var_up_out, mom_down_out, var_down_out, gp_hbm,
                h, g, wu, wd, pu, pd, act, dz, ut0, gp, tile, tiles,
                own, pair, rb1, part1, rb2, part2, rb3, red, gath,
                in_sem, gp_sem, out_sem, pair_send, pair_recv, rs_send, rs_recv, ag_send, ag_recv,
                swap_send, swap_recv):
    torus = Torus()
    net = Reducer(torus, tiles, own, pair, rb1, part1, rb2, part2, rb3, red, gath,
                  (pair_send, pair_recv, rs_send, rs_recv, ag_send, ag_recv, swap_send, swap_recv))
    state = ((mom_up, var_up, mom_up_out, var_up_out), (mom_down, var_down, mom_down_out, var_down_out))

    outs = []

    def result(m):
        net.arrive(("swap", m))
        cp = pltpu.make_async_copy(gath.at[m], dir_out.at[m], out_sem.at[m])
        cp.start()
        outs.append(cp)

    def update(m):
        net.collect(2, m)
        mom, var, mom_out, var_out = state[m % 2]
        mom_out[m // 2], var_out[m // 2] = net.update(m, mom[m // 2], var[m // 2])
        net.spread(0, m)

    moves = {
        "begin": net.begin, "all": net.begin_all, "line": lambda m: net.step(0, m), "plane": lambda m: net.step(1, m), "adam": update,
        "pass": lambda m: net.pass_on(0, m), "fan": lambda m: net.pass_on(1, m), "swap": net.swap, "out": result,
    }

    def play(names):
        for name in names.split():
            with jax.named_scope(name):
                moves[name[:-1]](int(name[-1]))

    def run(name, body, start, stop):
        with jax.named_scope(name):
            lax.fori_loop(start, stop, body, 0)

    ut1, vt = wu.at[0, 0:256], wu.at[0, 256:512]
    loads = {}

    def load(name, src, dst):
        cp = pltpu.make_async_copy(src, dst, in_sem.at[len(loads)])
        cp.start()
        loads[name] = cp

    load("x", x_hbm, h)
    load("wu0", wu_hbm.at[0], wu.at[0])
    load("pu", pu_hbm, pu)
    load("wd0", wd_hbm.at[0], wd.at[0])
    load("dh", dh_hbm, g)
    load("pd", pd_hbm, pd)
    load("wu1", wu_hbm.at[1], wu.at[1])
    load("wd1", wd_hbm.at[1], wd.at[1])

    def slope_out(rb, half):
        part = pl.ds(2 * half, 2)
        return pltpu.make_async_copy(own.at[part], gp_hbm.at[rb, part], gp_sem.at[half])

    def slope_in(n, half):
        return pltpu.make_async_copy(gp_hbm.at[:, n // 2, pl.ds(2 * lax.rem(n, 2), 2)], gp.at[half], gp_sem.at[half])

    for name in ("x", "wu0", "pu"):
        loads[name].wait()

    def forward_zero(rb, _):
        rows = block_rows(rb)
        for half in range(2):
            @pl.when(rb > 0)
            def _():
                slope_out(rb - 1, half).wait()

            for n in range(4 * half, 4 * half + 4):
                cols = slice(TILE * n, TILE * n + TILE)
                value, slope = gelu_pair(dot(h[rows], wu[0, :, cols]))
                act[rows, cols] = value.astype(BF16)
                own[n // 2, 2 * (n % 2):2 * (n % 2) + 2] = slope.reshape(PIECE)
            if half == 0:
                ut0[:, rows] = dot(h[rows], pu[0]).astype(BF16).T
            slope_out(rb, half).start()

        @pl.when(rb == 0)
        def _():
            loads["wd0"].wait()

        for k in range(3):
            cols = slice(256 * k, 256 * k + 256)
            h[rows, cols] = (h[rows, cols] + dot(act[rows], wd[0, :, cols])).astype(BF16)
        return 0

    run("fwd0", forward_zero, 0, BLOCKS)
    for name in ("dh", "pd", "wu1", "wd1"):
        loads[name].wait()
    peers_ready = entry_barrier(torus)
    for half in range(2):
        slope_out(BLOCKS - 1, half).wait()

    def project_one(rb, _):
        rows = block_rows(rb)
        ut1[:, rows] = dot(h[rows], pu[1]).astype(BF16).T
        vt[:, rows] = dot(g[rows], pd[1]).astype(BF16).T
        return 0

    run("proj1", project_one, 0, BLOCKS)

    def layer_one(n, _):
        cols = tile_cols(n)
        slot = 2 * lax.rem(n, 2)

        @pl.when(n >= 2)
        def _():
            net.pair_copy(3, n - 2, slot).wait_send()
            net.pair_copy(2, n - 2, slot + 1).wait_send()

        @pl.when((n >= 3) & (lax.rem(n, 2) == 1))
        def _():
            net.slab(3, n // 2 - 1)
            net.slab(2, n // 2 - 1)

        for rc in range(BLOCKS):
            rows = slice(BLOCK * rc, BLOCK * rc + BLOCK)
            value, slope = gelu_pair(dot(h[rows], wu[1, :, cols]))
            tile[rows] = value.astype(BF16)
            dz[rows, cols] = (slope * dot_t(g[rows], wd[1, cols, :])).astype(BF16)
        net.emit(3, n, slot, dot(vt[...], tile[...]))
        net.emit(2, n, slot + 1, dot(ut1[...], dz[:, cols]))
        return 0

    peers_ready()
    run("layer1", layer_one, 0, TILES)

    def input_grad(rb, _):
        rows = block_rows(rb)
        for k in range(3):
            cols = slice(256 * k, 256 * k + 256)
            g[rows, cols] = (g[rows, cols] + dot_t(dz[rows], wu[1, cols, :])).astype(BF16)
        vt[:, rows] = dot(g[rows], pd[0]).astype(BF16).T
        return 0

    run("g1a", input_grad, 0, 1)
    play("begin3 begin2")
    run("g1b", input_grad, 1, BLOCKS)
    for n in (TILES - 2, TILES - 1):
        net.pair_copy(3, n, 2 * (n % 2)).wait_send()
        net.pair_copy(2, n, 2 * (n % 2) + 1).wait_send()

    def down_zero(n, _):
        slot = lax.rem(n, 4)

        @pl.when(n >= 4)
        def _():
            net.pair_copy(1, n - 4, slot).wait_send()

        net.emit(1, n, slot, dot(vt[...], act[:, tile_cols(n)]))
        return 0

    slope_in(0, 0).start()
    run("down0", down_zero, 0, TILES)
    for n in range(4, TILES):
        net.pair_copy(1, n, n % 4).wait_send()

    def up_rows(n):
        half = lax.rem(n, 2)
        slope_in(n, half).wait()

        @pl.when(n < TILES - 1)
        def _():
            slope_in(n + 1, 1 - half).start()

        for rc in range(BLOCKS):
            rows = slice(BLOCK * rc, BLOCK * rc + BLOCK)
            d_act = dot_t(g[rows], wd[0, tile_cols(n), :])
            h[rows, tile_cols(half)] = (gp[half, rc].reshape(BLOCK, TILE) * d_act).astype(BF16)

    def up_sum(n):
        net.emit(0, n, lax.rem(n, 4), dot(ut0[...], h[:, tile_cols(lax.rem(n, 2))]))

    def up_zero(n, _):
        @pl.when(n >= 5)
        def _():
            net.pair_copy(0, n - 5, lax.rem(n - 1, 4)).wait_send()

        @pl.when((n >= 4) & (lax.rem(n, 2) == 0))
        def _():
            net.slab(0, n // 2 - 2)

        up_rows(n)
        up_sum(n - 1)
        return 0

    up_rows(0)
    first = 1
    for last, names in SCHEDULE:
        run(f"up{first}", up_zero, first, last)
        play(names)
        first = last
    net.pair_copy(0, 3, 3).wait_send()
    up_sum(TILES - 1)
    net.slab(0, 2)
    for names in LAST:
        play(names)
    for names in TAIL:
        play(names)
    for n in range(4, TILES):
        net.pair_copy(0, n, n % 4).wait_send()
    net.finish()
    play("out1 out0")
    for cp in outs:
        cp.wait()


def train_step(x_rows, dh_rows, w_up, w_down, proj_up, proj_down, moments):
    hbm = pl.BlockSpec(memory_space=pl.ANY)
    vmem = pl.BlockSpec(memory_space=pltpu.VMEM)
    dma = pltpu.SemaphoreType.DMA
    shard = jax.ShapeDtypeStruct((2, 16, RANK), F32)

    def sums(lines, *lead):
        return pltpu.VMEM(lead + (4,) * lines + (2, 8, RANK), F32)

    return pl.pallas_call(
        step_kernel,
        out_shape=(jax.ShapeDtypeStruct(DIRECTIONS, BF16),) + (shard,) * 4
        + (jax.ShapeDtypeStruct((BLOCKS, 4) + (4,) * 3 + (2, 8, RANK), F32),),
        in_specs=[hbm] * 6 + [vmem] * 4,
        out_specs=(hbm,) + (vmem,) * 4 + (hbm,),
        scratch_shapes=[
            pltpu.VMEM((ROWS, WIDTH), BF16),
            pltpu.VMEM((ROWS, WIDTH), BF16),
            pltpu.VMEM(w_up.shape, BF16),
            pltpu.VMEM(w_down.shape, BF16),
            pltpu.VMEM(proj_up.shape, BF16),
            pltpu.VMEM(proj_down.shape, BF16),
            pltpu.VMEM((ROWS, FF), BF16),
            pltpu.VMEM((ROWS, FF), BF16),
            pltpu.VMEM((RANK, ROWS), BF16),
            pltpu.VMEM((2, BLOCKS) + PIECE, F32),
            pltpu.VMEM((ROWS, TILE), BF16),
            pltpu.VMEM((4, 2, 4, 2, 2, 8, RANK), F32),
            sums(3, 4), sums(3, 4),
            sums(2, 4, 3), sums(2, 4),
            sums(1, 4, 3), sums(1, 4),
            sums(0, 4, 3),
            pltpu.VMEM((4, 16, RANK), F32),
            pltpu.VMEM(DIRECTIONS, BF16),
            dma((8,)), dma((2,)), dma((4,)), dma((4,)), dma((4, TILES)),
            dma((3, 4, 3, 3)), dma((3, 4, 3, 3)),
            dma((3, 4, 2, 3)), dma((3, 4, 2, 3)),
            dma((4,)), dma((4,)),
        ],
        compiler_params=pltpu.CompilerParams(
            collective_id=0, has_side_effects=True, vmem_limit_bytes=67_043_328),
    )(x_rows, dh_rows, w_up, w_down, proj_up, proj_down, *moments)


def weight_kernel(dir_up, dir_down, w_up, w_down, proj_up, proj_down, *refs):
    moments, new_up, new_down, outs = refs[:4], refs[4], refs[5], refs[6:]

    @pl.when((pl.program_id(0) == 0) & (pl.program_id(1) == 0))
    def _():
        for src, dst in zip(moments, outs):
            dst[...] = src[...]

    new_up[0] = (w_up[0] - SCALE * dot_t(proj_up[0], dir_up[0])).astype(BF16)
    new_down[0] = (w_down[0] - SCALE * dot_t(dir_down[0], proj_down[0])).astype(BF16)


def new_weights(directions, w_up, w_down, proj_up, proj_down, moments):
    width = 512
    up_spec = pl.BlockSpec((1, 768, width), lambda l, n: (l, 0, n))
    down_spec = pl.BlockSpec((1, width, 768), lambda l, n: (l, n, 0))
    proj_spec = pl.BlockSpec((1, 768, 256), lambda l, n: (l, 0, 0))
    shard_spec = pl.BlockSpec((2, 16, 256), lambda l, n: (0, 0, 0))
    return pl.pallas_call(
        weight_kernel,
        grid=(2, 2048 // width),
        out_shape=(jax.ShapeDtypeStruct(w_up.shape, BF16), jax.ShapeDtypeStruct(w_down.shape, BF16))
        + (jax.ShapeDtypeStruct((2, 16, 256), F32),) * 4,
        in_specs=[
            pl.BlockSpec((1, width, 256), lambda l, n: (2 * l, n, 0)),
            pl.BlockSpec((1, width, 256), lambda l, n: (2 * l + 1, n, 0)),
            up_spec, down_spec, proj_spec, proj_spec,
        ] + [shard_spec] * 4,
        out_specs=(up_spec, down_spec) + (shard_spec,) * 4,
    )(directions, directions, w_up, w_down, proj_up, proj_down, *moments)


def solution(mesh):
    def local_step(x_loc, dh_loc, w_up, w_down, proj_up, proj_down, mom_up, var_up, mom_down, var_down):
        moments = (jnp.swapaxes(mom_up, 1, 2), jnp.swapaxes(var_up, 1, 2), mom_down, var_down)
        directions, *moments, _ = train_step(x_loc, dh_loc, w_up, w_down, proj_up, proj_down, moments)
        new_up, new_down, *moments = new_weights(
            directions.reshape(4, 2048, 256), w_up, w_down, proj_up, proj_down, moments)
        return (new_up, new_down, jnp.swapaxes(moments[0], 1, 2), jnp.swapaxes(moments[1], 1, 2), moments[2], moments[3])

    tok_spec = P('data', None)
    up_spec = P(None, None, 'data')
    down_spec = P(None, 'data', None)
    return jax.shard_map(
        local_step,
        mesh=mesh,
        in_specs=(tok_spec, tok_spec, P(), P(), P(), P(), up_spec, up_spec, down_spec, down_spec),
        out_specs=(P(), P(), up_spec, up_spec, down_spec, down_spec),
        check_vma=False,
    )
```

```python
import jax
import jax.numpy as jnp
from jax import lax
from jax.experimental import pallas as pl
from jax.experimental.pallas import tpu as pltpu
from jax.sharding import PartitionSpec as P

BETA_ONE = 0.9
BETA_TWO = 0.999
EPSILON = 1e-8
STEP = 4
LEARN_RATE = 0.02
ALPHA_SCALE = 0.25
SCALE = LEARN_RATE * ALPHA_SCALE
GELU_A = 0.7978845608028654
GELU_B = 0.044715
MESH = pl.DeviceIdType.MESH
ALL = slice(None)
ROWS, WIDTH, FF, RANK = 2048, 768, 2048, 256
F32, BF16 = jnp.float32, jnp.bfloat16

PIECE = (2, 4, 4, 2, 8, RANK)
DIRECTIONS = (4,) * 4 + (2, 16, RANK)
BLOCK = 512
TILE = 256
BLOCKS = 4
TILES = 8

ORDERS = ((2, 1, 0), (1, 0, 2), (0, 2, 1))
COLOURS = ((0, 1, 2), (1, 2, 0), (2, 0, 1), (0, 1, 2))
PIECES = ((0, 0, 256), (1, 0, 128), (1, 128, 128))
UNITS = ((0, 1), (2, 0), (1, 2), (0, 1))
SCHEDULE = (
    (2, "adam3 adam2"),
    (4, "pass3 pass2"),
    (6, "line1 fan3 fan2"),
    (8, "plane1"),
)
LAST = ("begin0 swap3 swap2 adam1",)
TAIL = ("line0 pass1 plane0 fan1", "adam0 pass0 out3 out2", "fan0 swap1")


def dot(lhs, rhs):
    return jnp.dot(lhs, rhs, preferred_element_type=F32)


def dot_t(lhs, rhs):
    return lax.dot_general(lhs, rhs, (((1,), (1,)), ((), ())), preferred_element_type=F32)


def gelu_pair(z):
    sq = z * z
    cdf = 0.5 + 0.5 * jnp.tanh(z * (GELU_A + (GELU_A * GELU_B) * sq))
    act = z * cdf
    slope = cdf + act * ((1.0 - cdf) * (2.0 * GELU_A + (6.0 * GELU_A * GELU_B) * sq))
    return act, slope


def adam_shard(moment, variance, grad_red):
    new_mom = BETA_ONE * moment + (1.0 - BETA_ONE) * grad_red
    new_var = BETA_TWO * variance + (1.0 - BETA_TWO) * grad_red * grad_red
    bias_one = 1.0 - BETA_ONE ** STEP
    bias_two = 1.0 - BETA_TWO ** STEP
    direction = (new_mom / bias_one) / (jnp.sqrt(new_var / bias_two) + EPSILON)
    return new_mom, new_var, direction.astype(BF16)


def block_rows(i):
    return pl.ds(pl.multiple_of(i * BLOCK, BLOCK), BLOCK)


def tile_cols(n):
    return pl.ds(pl.multiple_of(n * TILE, TILE), TILE)


class Torus:
    def __init__(self):
        me = lax.axis_index("data")
        self.core = lax.rem(me, 2)
        chip = me // 2
        self.coords = (chip // 16, lax.rem(chip // 4, 4), lax.rem(chip, 4))
        self.partner = me + 1 - 2 * self.core

    def coord(self, axis, offset):
        return lax.rem(self.coords[axis] + offset, 4)

    def peer(self, axis, offset):
        z, y, x = (self.coord(a, offset) if a == axis else self.coords[a] for a in range(3))
        return ((z * 4 + y) * 4 + x) * 2 + self.core


def remote(src, dst, send_sem, recv_sem, device):
    return pltpu.make_async_remote_copy(
        src_ref=src, dst_ref=dst, send_sem=send_sem, recv_sem=recv_sem,
        device_id=(device,), device_id_type=MESH,
    )


def entry_barrier(torus):
    barrier = pltpu.get_barrier_semaphore()
    pl.semaphore_signal(barrier, inc=1, device_id=(torus.partner,), device_id_type=MESH)
    for axis in range(3):
        for offset in (1, 2, 3):
            pl.semaphore_signal(barrier, inc=1, device_id=(torus.peer(axis, offset),), device_id_type=MESH)
    return lambda: pl.semaphore_wait(barrier, 10)


def at_axis(axes, axis, index):
    return tuple(index if a == axis else ALL for a in axes)


class Reducer:
    def __init__(self, torus, tiles, own, pair, rb1, part1, rb2, part2, rb3, red, gath, sems):
        self.torus = torus
        self.tiles = tiles
        self.src = (own, part1, part2)
        self.got = (rb1, rb2, rb3)
        self.pair, self.red, self.gath = pair, red, gath
        (self.pair_send, self.pair_recv, self.rs_send, self.rs_recv, self.ag_send, self.ag_recv, self.swap_send,
         self.swap_recv) = sems
        self.pending = []
        self.inbound = {}

    def pair_copy(self, m, n, slot):
        where = (m, n // 2, pl.ds(2 * lax.rem(n, 2), 2))
        return remote(self.tiles.at[slot, :, :, 1 - self.torus.core], self.pair.at[where],
                      self.pair_send.at[slot], self.pair_recv.at[m, n], self.torus.partner)

    def emit(self, m, n, slot, part):
        self.tiles[slot] = part.T.reshape(2, 4, 2, 2, 8, 256)
        self.src[0][m, n // 2, pl.ds(2 * lax.rem(n, 2), 2)] = self.tiles[slot, :, :, self.torus.core]
        self.pair_copy(m, n, slot).start()

    def slab(self, m, z):
        own, pair = self.src[0], self.pair
        for half in range(2):
            self.pair_copy(m, 2 * z + half, 0).wait_recv()
        own[m, z] = own[m, z] + pair[m, z]
        for k, (half, lane, width) in enumerate(PIECES):
            axis = ORDERS[COLOURS[m][k]][0]
            tail = (half, ALL, pl.ds(lane, width))
            if axis == 0:
                offset = lax.rem(z + 4 - self.torus.coords[0], 4)

                @pl.when(offset > 0)
                def _():
                    self.copy(own.at[(m, z) + (ALL,) * 2 + tail],
                              self.got[0].at[(m, offset - 1) + (ALL,) * 2 + tail],
                              (0, m, k, offset - 1), self.torus.peer(0, offset)).start()
                continue
            for offset in (1, 2, 3):
                where = at_axis((1, 2), axis, self.torus.coord(axis, offset))
                self.copy(own.at[(m, z) + where + tail], self.got[0].at[(m, offset - 1, z, ALL) + tail],
                          (0, m, k, offset - 1), self.torus.peer(axis, offset)).start()

    def begin(self, m):
        self.slab(m, 3)
        self.scatter(0, m, False)

    def begin_all(self, m):
        lax.fori_loop(0, 3, lambda z, _: (self.slab(m, z), 0)[1], 0)
        self.begin(m)

    def copy(self, src, dst, sem, device):
        return remote(src, dst, self.rs_send.at[sem], self.rs_recv.at[sem], device)

    def step(self, phase, m):
        self.collect(phase, m)
        self.scatter(phase + 1, m)

    def pass_on(self, phase, m):
        self.spread_arrive(phase, m)
        self.spread(phase + 1, m)

    def start(self, cp, key, go=True):
        if go:
            cp.start()
        self.pending.append(cp)
        self.inbound.setdefault(key, []).append(cp)

    def arrive(self, key):
        for cp in self.inbound[key]:
            cp.wait_recv()

    def scatter(self, phase, m, go=True):
        for k, (half, lane, width) in enumerate(PIECES):
            order = ORDERS[COLOURS[m][k]]
            axis = order[phase]
            axes = tuple(a for a in range(3) if a not in order[:phase])
            tail = (half, ALL, pl.ds(lane, width))
            for offset in (1, 2, 3):
                where = at_axis(axes, axis, self.torus.coord(axis, offset))
                rest = (ALL,) * (len(axes) - 1)
                self.start(self.copy(
                    self.src[phase].at[(m,) + where + tail], self.got[phase].at[(m, offset - 1) + rest + tail],
                    (phase, m, k, offset - 1), self.torus.peer(axis, offset)), ("rs", phase, m, k), go)

    def collect(self, phase, m):
        for k, (half, lane, width) in enumerate(PIECES):
            order = ORDERS[COLOURS[m][k]]
            axis = order[phase]
            axes = tuple(a for a in range(3) if a not in order[:phase])
            tail = (half, ALL, slice(lane, lane + width))
            rest = (ALL,) * (len(axes) - 1)
            self.arrive(("rs", phase, m, k))
            got = self.got[phase]
            total = self.src[phase][(m,) + at_axis(axes, axis, self.torus.coords[axis]) + tail]
            for other in range(3):
                total = total + got[(m, other) + rest + tail]
            if phase < 2:
                self.src[phase + 1][(m,) + rest + tail] = total
            else:
                self.red[m, 8 * half:8 * half + 8, lane:lane + width] = total

    def update(self, m, moment, variance):
        z, y, x = self.torus.coords
        new_mom, new_var, direction = adam_shard(moment, variance, self.red[m])
        self.gath[m, z, y, x, self.torus.core] = direction
        return new_mom, new_var

    def spread(self, phase, m):
        for j in range(2):
            order = ORDERS[UNITS[m][j]][::-1]
            axis = order[phase]
            where = tuple(ALL if a in order[:phase] else self.torus.coords[a] for a in range(3))
            ref = self.gath.at[(m,) + where + (self.torus.core, ALL, pl.ds(128 * j, 128))]
            for offset in (1, 2, 3):
                self.start(remote(
                    ref, ref, self.ag_send.at[phase, m, j, offset - 1], self.ag_recv.at[phase, m, j, offset - 1],
                    self.torus.peer(axis, offset)), ("ag", phase, m))

    def spread_arrive(self, phase, m):
        self.arrive(("ag", phase, m))

    def swap(self, m):
        self.spread_arrive(2, m)
        ref = self.gath.at[m, :, :, :, self.torus.core]
        self.start(remote(ref, ref, self.swap_send.at[m], self.swap_recv.at[m], self.torus.partner), ("swap", m))

    def finish(self):
        for cp in self.pending:
            cp.wait_send()
        self.pending = []


def step_kernel(x_hbm, dh_hbm, wu_hbm, wd_hbm, pu_hbm, pd_hbm, mom_up, var_up, mom_down, var_down,
                dir_out, state_out, gp_hbm,
                h, g, wu, wd, pu, pd, act, dz, ut0, gp, tile, tiles,
                own, pair, rb1, part1, rb2, part2, rb3, red, gath, fresh,
                in_sem, gp_sem, out_sem, state_sem, pair_send, pair_recv, rs_send, rs_recv, ag_send, ag_recv,
                swap_send, swap_recv):
    torus = Torus()
    net = Reducer(torus, tiles, own, pair, rb1, part1, rb2, part2, rb3, red, gath,
                  (pair_send, pair_recv, rs_send, rs_recv, ag_send, ag_recv, swap_send, swap_recv))
    state = ((mom_up, var_up), (mom_down, var_down))

    outs = []

    def result(m):
        net.arrive(("swap", m))
        cp = pltpu.make_async_copy(gath.at[m], dir_out.at[m], out_sem.at[m])
        cp.start()
        outs.append(cp)

    def update(m):
        net.collect(2, m)
        mom, var = state[m % 2]
        fresh[m, 0], fresh[m, 1] = net.update(m, mom[m // 2], var[m // 2])
        net.spread(0, m)
        cp = pltpu.make_async_copy(fresh.at[m], state_out.at[m], state_sem.at[m])
        cp.start()
        outs.append(cp)

    moves = {
        "begin": net.begin, "all": net.begin_all, "line": lambda m: net.step(0, m), "plane": lambda m: net.step(1, m), "adam": update,
        "pass": lambda m: net.pass_on(0, m), "fan": lambda m: net.pass_on(1, m), "swap": net.swap, "out": result,
    }

    def play(names):
        for name in names.split():
            with jax.named_scope(name):
                moves[name[:-1]](int(name[-1]))

    def run(name, body, start, stop):
        with jax.named_scope(name):
            lax.fori_loop(start, stop, body, 0)

    ut1, vt = wu.at[0, 0:256], wu.at[0, 256:512]
    loads = {}

    def load(name, src, dst):
        cp = pltpu.make_async_copy(src, dst, in_sem.at[len(loads)])
        cp.start()
        loads[name] = cp

    load("x", x_hbm, h)
    load("wu0", wu_hbm.at[0], wu.at[0])
    load("pu", pu_hbm, pu)
    load("wd0", wd_hbm.at[0], wd.at[0])
    load("dh", dh_hbm, g)
    load("pd", pd_hbm, pd)
    load("wu1", wu_hbm.at[1], wu.at[1])
    load("wd1", wd_hbm.at[1], wd.at[1])

    def slope_out(rb, half):
        part = pl.ds(2 * half, 2)
        return pltpu.make_async_copy(own.at[part], gp_hbm.at[rb, part], gp_sem.at[half])

    def slope_in(n, half):
        return pltpu.make_async_copy(gp_hbm.at[:, n // 2, pl.ds(2 * lax.rem(n, 2), 2)], gp.at[half], gp_sem.at[half])

    for name in ("x", "wu0", "pu"):
        loads[name].wait()

    def forward_zero(rb, _):
        rows = block_rows(rb)
        for half in range(2):
            @pl.when(rb > 0)
            def _():
                slope_out(rb - 1, half).wait()

            for n in range(4 * half, 4 * half + 4):
                cols = slice(TILE * n, TILE * n + TILE)
                value, slope = gelu_pair(dot(h[rows], wu[0, :, cols]))
                act[rows, cols] = value.astype(BF16)
                own[n // 2, 2 * (n % 2):2 * (n % 2) + 2] = slope.reshape(PIECE)
            if half == 0:
                ut0[:, rows] = dot(h[rows], pu[0]).astype(BF16).T
            slope_out(rb, half).start()

        @pl.when(rb == 0)
        def _():
            loads["wd0"].wait()

        for k in range(3):
            cols = slice(256 * k, 256 * k + 256)
            h[rows, cols] = (h[rows, cols] + dot(act[rows], wd[0, :, cols])).astype(BF16)
        return 0

    run("fwd0", forward_zero, 0, BLOCKS)
    for name in ("dh", "pd", "wu1", "wd1"):
        loads[name].wait()
    peers_ready = entry_barrier(torus)
    for half in range(2):
        slope_out(BLOCKS - 1, half).wait()

    def project_one(rb, _):
        rows = block_rows(rb)
        ut1[:, rows] = dot(h[rows], pu[1]).astype(BF16).T
        vt[:, rows] = dot(g[rows], pd[1]).astype(BF16).T
        return 0

    run("proj1", project_one, 0, BLOCKS)

    def layer_one(n, _):
        cols = tile_cols(n)
        slot = 2 * lax.rem(n, 2)

        @pl.when(n >= 2)
        def _():
            net.pair_copy(3, n - 2, slot).wait_send()
            net.pair_copy(2, n - 2, slot + 1).wait_send()

        @pl.when((n >= 3) & (lax.rem(n, 2) == 1))
        def _():
            net.slab(3, n // 2 - 1)
            net.slab(2, n // 2 - 1)

        for rc in range(BLOCKS):
            rows = slice(BLOCK * rc, BLOCK * rc + BLOCK)
            value, slope = gelu_pair(dot(h[rows], wu[1, :, cols]))
            tile[rows] = value.astype(BF16)
            dz[rows, cols] = (slope * dot_t(g[rows], wd[1, cols, :])).astype(BF16)
        net.emit(3, n, slot, dot(vt[...], tile[...]))
        net.emit(2, n, slot + 1, dot(ut1[...], dz[:, cols]))
        return 0

    peers_ready()
    run("layer1", layer_one, 0, TILES)

    def input_grad(rb, _):
        rows = block_rows(rb)
        for k in range(3):
            cols = slice(256 * k, 256 * k + 256)
            g[rows, cols] = (g[rows, cols] + dot_t(dz[rows], wu[1, cols, :])).astype(BF16)
        vt[:, rows] = dot(g[rows], pd[0]).astype(BF16).T
        return 0

    run("g1a", input_grad, 0, 1)
    play("begin3 begin2")
    run("g1b", input_grad, 1, BLOCKS)
    play("line3 line2")
    for n in (TILES - 2, TILES - 1):
        net.pair_copy(3, n, 2 * (n % 2)).wait_send()
        net.pair_copy(2, n, 2 * (n % 2) + 1).wait_send()

    def down_zero(n, _):
        slot = lax.rem(n, 4)

        @pl.when(n >= 4)
        def _():
            net.pair_copy(1, n - 4, slot).wait_send()

        net.emit(1, n, slot, dot(vt[...], act[:, tile_cols(n)]))
        return 0

    slope_in(0, 0).start()
    run("down0", down_zero, 0, TILES)
    for n in range(4, TILES):
        net.pair_copy(1, n, n % 4).wait_send()

    def up_rows(n):
        half = lax.rem(n, 2)
        slope_in(n, half).wait()

        @pl.when(n < TILES - 1)
        def _():
            slope_in(n + 1, 1 - half).start()

        for rc in range(BLOCKS):
            rows = slice(BLOCK * rc, BLOCK * rc + BLOCK)
            d_act = dot_t(g[rows], wd[0, tile_cols(n), :])
            h[rows, tile_cols(half)] = (gp[half, rc].reshape(BLOCK, TILE) * d_act).astype(BF16)

    def up_sum(n):
        net.emit(0, n, lax.rem(n, 4), dot(ut0[...], h[:, tile_cols(lax.rem(n, 2))]))

    def up_zero(n, _):
        @pl.when(n >= 5)
        def _():
            net.pair_copy(0, n - 5, lax.rem(n - 1, 4)).wait_send()

        @pl.when((n >= 4) & (lax.rem(n, 2) == 0))
        def _():
            net.slab(0, n // 2 - 2)

        up_rows(n)
        up_sum(n - 1)
        return 0

    play("plane3 plane2 all1")
    up_rows(0)
    first = 1
    for last, names in SCHEDULE:
        run(f"up{first}", up_zero, first, last)
        play(names)
        first = last
    net.pair_copy(0, 3, 3).wait_send()
    up_sum(TILES - 1)
    net.slab(0, 2)
    for names in LAST:
        play(names)
    for names in TAIL:
        play(names)
    for n in range(4, TILES):
        net.pair_copy(0, n, n % 4).wait_send()
    net.finish()
    play("swap0 out1 out0")
    net.finish()
    for cp in outs:
        cp.wait()


def train_step(x_rows, dh_rows, w_up, w_down, proj_up, proj_down, moments):
    hbm = pl.BlockSpec(memory_space=pl.ANY)
    vmem = pl.BlockSpec(memory_space=pltpu.VMEM)
    dma = pltpu.SemaphoreType.DMA

    def sums(lines, *lead):
        return pltpu.VMEM(lead + (4,) * lines + (2, 8, RANK), F32)

    return pl.pallas_call(
        step_kernel,
        out_shape=(jax.ShapeDtypeStruct(DIRECTIONS, BF16), jax.ShapeDtypeStruct((4, 2, 16, RANK), F32),
                   jax.ShapeDtypeStruct((BLOCKS, 4) + (4,) * 3 + (2, 8, RANK), F32)),
        in_specs=[hbm] * 6 + [vmem] * 4,
        out_specs=(hbm,) * 3,
        scratch_shapes=[
            pltpu.VMEM((ROWS, WIDTH), BF16),
            pltpu.VMEM((ROWS, WIDTH), BF16),
            pltpu.VMEM(w_up.shape, BF16),
            pltpu.VMEM(w_down.shape, BF16),
            pltpu.VMEM(proj_up.shape, BF16),
            pltpu.VMEM(proj_down.shape, BF16),
            pltpu.VMEM((ROWS, FF), BF16),
            pltpu.VMEM((ROWS, FF), BF16),
            pltpu.VMEM((RANK, ROWS), BF16),
            pltpu.VMEM((2, BLOCKS) + PIECE, F32),
            pltpu.VMEM((ROWS, TILE), BF16),
            pltpu.VMEM((4, 2, 4, 2, 2, 8, RANK), F32),
            sums(3, 4), sums(3, 4),
            sums(2, 4, 3), sums(2, 4),
            sums(1, 4, 3), sums(1, 4),
            sums(0, 4, 3),
            pltpu.VMEM((4, 16, RANK), F32),
            pltpu.VMEM(DIRECTIONS, BF16),
            pltpu.VMEM((4, 2, 16, RANK), F32),
            dma((8,)), dma((2,)), dma((4,)), dma((4,)), dma((4,)), dma((4, TILES)),
            dma((3, 4, 3, 3)), dma((3, 4, 3, 3)),
            dma((3, 4, 2, 3)), dma((3, 4, 2, 3)),
            dma((4,)), dma((4,)),
        ],
        compiler_params=pltpu.CompilerParams(
            collective_id=0, has_side_effects=True, vmem_limit_bytes=67_043_328),
    )(x_rows, dh_rows, w_up, w_down, proj_up, proj_down, *moments)


def weight_kernel(dir_up, dir_down, w_up, w_down, proj_up, proj_down, *refs):
    state, new_up, new_down, outs = refs[0], refs[1], refs[2], refs[3:]

    @pl.when((pl.program_id(0) == 0) & (pl.program_id(1) == 0))
    def _():
        for m in range(4):
            for k in range(2):
                outs[2 * (m % 2) + k][m // 2] = state[m, k]

    new_up[0] = (w_up[0] - SCALE * dot_t(proj_up[0], dir_up[0])).astype(BF16)
    new_down[0] = (w_down[0] - SCALE * dot_t(dir_down[0], proj_down[0])).astype(BF16)


def new_weights(directions, w_up, w_down, proj_up, proj_down, state):
    width = 512
    up_spec = pl.BlockSpec((1, 768, width), lambda l, n: (l, 0, n))
    down_spec = pl.BlockSpec((1, width, 768), lambda l, n: (l, n, 0))
    proj_spec = pl.BlockSpec((1, 768, 256), lambda l, n: (l, 0, 0))
    shard_spec = pl.BlockSpec((2, 16, 256), lambda l, n: (0, 0, 0))
    return pl.pallas_call(
        weight_kernel,
        grid=(2, 2048 // width),
        out_shape=(jax.ShapeDtypeStruct(w_up.shape, BF16), jax.ShapeDtypeStruct(w_down.shape, BF16))
        + (jax.ShapeDtypeStruct((2, 16, 256), F32),) * 4,
        in_specs=[
            pl.BlockSpec((1, width, 256), lambda l, n: (2 * l, n, 0)),
            pl.BlockSpec((1, width, 256), lambda l, n: (2 * l + 1, n, 0)),
            up_spec, down_spec, proj_spec, proj_spec,
            pl.BlockSpec(state.shape, lambda l, n: (0, 0, 0, 0)),
        ],
        out_specs=(up_spec, down_spec) + (shard_spec,) * 4,
    )(directions, directions, w_up, w_down, proj_up, proj_down, state)


def solution(mesh):
    def local_step(x_loc, dh_loc, w_up, w_down, proj_up, proj_down, mom_up, var_up, mom_down, var_down):
        moments = (jnp.swapaxes(mom_up, 1, 2), jnp.swapaxes(var_up, 1, 2), mom_down, var_down)
        directions, state, _ = train_step(x_loc, dh_loc, w_up, w_down, proj_up, proj_down, moments)
        new_up, new_down, *moments = new_weights(
            directions.reshape(4, 2048, 256), w_up, w_down, proj_up, proj_down, state)
        return (new_up, new_down, jnp.swapaxes(moments[0], 1, 2), jnp.swapaxes(moments[1], 1, 2), moments[2], moments[3])

    tok_spec = P('data', None)
    up_spec = P(None, None, 'data')
    down_spec = P(None, 'data', None)
    return jax.shard_map(
        local_step,
        mesh=mesh,
        in_specs=(tok_spec, tok_spec, P(), P(), P(), P(), up_spec, up_spec, down_spec, down_spec),
        out_specs=(P(), P(), up_spec, up_spec, down_spec, down_spec),
        check_vma=False,
    )
```

```python
import jax
import jax.numpy as jnp
from jax import lax
from jax.experimental import pallas as pl
from jax.experimental.pallas import tpu as pltpu
from jax.sharding import PartitionSpec as P

BETA_ONE = 0.9
BETA_TWO = 0.999
EPSILON = 1e-8
STEP = 4
LEARN_RATE = 0.02
ALPHA_SCALE = 0.25
SCALE = LEARN_RATE * ALPHA_SCALE
GELU_A = 0.7978845608028654
GELU_B = 0.044715
MESH = pl.DeviceIdType.MESH
ALL = slice(None)
ROWS, WIDTH, FF, RANK = 2048, 768, 2048, 256
F32, BF16 = jnp.float32, jnp.bfloat16

PIECE = (2, 4, 4, 2, 8, RANK)
DIRECTIONS = (4,) * 4 + (2, 16, RANK)
BLOCK = 512
TILE = 256
BLOCKS = 4
TILES = 8

ORDERS = ((2, 1, 0), (1, 0, 2), (0, 2, 1))
COLOURS = ((0, 1, 2), (1, 2, 0), (2, 0, 1), (0, 1, 2))
PIECES = ((0, 0, 256), (1, 0, 128), (1, 128, 128))
UNITS = ((0, 1), (2, 0), (1, 2), (0, 1))
SCHEDULE = (
    (2, "adam3 adam2"),
    (4, "pass3 pass2"),
    (6, "line1 fan3 fan2"),
    (8, "plane1"),
)
LAST = ("begin0 swap3 swap2 adam1",)
TAIL = ("line0 pass1 plane0 fan1", "adam0 pass0 out3 out2", "fan0 swap1")


def dot(lhs, rhs):
    return jnp.dot(lhs, rhs, preferred_element_type=F32)


def dot_t(lhs, rhs):
    return lax.dot_general(lhs, rhs, (((1,), (1,)), ((), ())), preferred_element_type=F32)


def gelu_pair(z):
    sq = z * z
    cdf = 0.5 + 0.5 * jnp.tanh(z * (GELU_A + (GELU_A * GELU_B) * sq))
    act = z * cdf
    slope = cdf + act * ((1.0 - cdf) * (2.0 * GELU_A + (6.0 * GELU_A * GELU_B) * sq))
    return act, slope


def adam_shard(moment, variance, grad_red):
    new_mom = BETA_ONE * moment + (1.0 - BETA_ONE) * grad_red
    new_var = BETA_TWO * variance + (1.0 - BETA_TWO) * grad_red * grad_red
    bias_one = 1.0 - BETA_ONE ** STEP
    bias_two = 1.0 - BETA_TWO ** STEP
    direction = (new_mom / bias_one) / (jnp.sqrt(new_var / bias_two) + EPSILON)
    return new_mom, new_var, direction.astype(BF16)


def block_rows(i):
    return pl.ds(pl.multiple_of(i * BLOCK, BLOCK), BLOCK)


def tile_cols(n):
    return pl.ds(pl.multiple_of(n * TILE, TILE), TILE)


class Torus:
    def __init__(self):
        me = lax.axis_index("data")
        self.core = lax.rem(me, 2)
        chip = me // 2
        self.coords = (chip // 16, lax.rem(chip // 4, 4), lax.rem(chip, 4))
        self.partner = me + 1 - 2 * self.core

    def coord(self, axis, offset):
        return lax.rem(self.coords[axis] + offset, 4)

    def peer(self, axis, offset):
        z, y, x = (self.coord(a, offset) if a == axis else self.coords[a] for a in range(3))
        return ((z * 4 + y) * 4 + x) * 2 + self.core


def remote(src, dst, send_sem, recv_sem, device):
    return pltpu.make_async_remote_copy(
        src_ref=src, dst_ref=dst, send_sem=send_sem, recv_sem=recv_sem,
        device_id=(device,), device_id_type=MESH,
    )


def entry_barrier(torus):
    barrier = pltpu.get_barrier_semaphore()
    pl.semaphore_signal(barrier, inc=1, device_id=(torus.partner,), device_id_type=MESH)
    for axis in range(3):
        for offset in (1, 2, 3):
            pl.semaphore_signal(barrier, inc=1, device_id=(torus.peer(axis, offset),), device_id_type=MESH)
    return lambda: pl.semaphore_wait(barrier, 10)


def at_axis(axes, axis, index):
    return tuple(index if a == axis else ALL for a in axes)


class Reducer:
    def __init__(self, torus, tiles, own, pair, rb1, part1, rb2, part2, rb3, red, gath, sems):
        self.torus = torus
        self.tiles = tiles
        self.src = (own, part1, part2)
        self.got = (rb1, rb2, rb3)
        self.pair, self.red, self.gath = pair, red, gath
        (self.pair_send, self.pair_recv, self.rs_send, self.rs_recv, self.ag_send, self.ag_recv, self.swap_send,
         self.swap_recv) = sems
        self.pending = []
        self.inbound = {}

    def pair_copy(self, m, n, slot):
        where = (m, n // 2, pl.ds(2 * lax.rem(n, 2), 2))
        return remote(self.tiles.at[slot, :, :, 1 - self.torus.core], self.pair.at[where],
                      self.pair_send.at[slot], self.pair_recv.at[m, n], self.torus.partner)

    def emit(self, m, n, slot, part):
        self.tiles[slot] = part.T.reshape(2, 4, 2, 2, 8, 256)
        self.src[0][m, n // 2, pl.ds(2 * lax.rem(n, 2), 2)] = self.tiles[slot, :, :, self.torus.core]
        self.pair_copy(m, n, slot).start()

    def slab(self, m, z):
        own, pair = self.src[0], self.pair
        for half in range(2):
            self.pair_copy(m, 2 * z + half, 0).wait_recv()
        own[m, z] = own[m, z] + pair[m, z]
        for k, (half, lane, width) in enumerate(PIECES):
            axis = ORDERS[COLOURS[m][k]][0]
            tail = (half, ALL, pl.ds(lane, width))
            if axis == 0:
                offset = lax.rem(z + 4 - self.torus.coords[0], 4)

                @pl.when(offset > 0)
                def _():
                    self.copy(own.at[(m, z) + (ALL,) * 2 + tail],
                              self.got[0].at[(m, offset - 1) + (ALL,) * 2 + tail],
                              (0, m, k, offset - 1), self.torus.peer(0, offset)).start()
                continue
            for offset in (1, 2, 3):
                where = at_axis((1, 2), axis, self.torus.coord(axis, offset))
                self.copy(own.at[(m, z) + where + tail], self.got[0].at[(m, offset - 1, z, ALL) + tail],
                          (0, m, k, offset - 1), self.torus.peer(axis, offset)).start()

    def begin(self, m):
        self.slab(m, 3)
        self.scatter(0, m, False)

    def begin_all(self, m):
        lax.fori_loop(0, 3, lambda z, _: (self.slab(m, z), 0)[1], 0)
        self.begin(m)

    def copy(self, src, dst, sem, device):
        return remote(src, dst, self.rs_send.at[sem], self.rs_recv.at[sem], device)

    def step(self, phase, m):
        self.collect(phase, m)
        self.scatter(phase + 1, m)

    def pass_on(self, phase, m):
        self.spread_arrive(phase, m)
        self.spread(phase + 1, m)

    def start(self, cp, key, go=True):
        if go:
            cp.start()
        self.pending.append(cp)
        self.inbound.setdefault(key, []).append(cp)

    def arrive(self, key):
        for cp in self.inbound[key]:
            cp.wait_recv()

    def scatter(self, phase, m, go=True):
        for k, (half, lane, width) in enumerate(PIECES):
            order = ORDERS[COLOURS[m][k]]
            axis = order[phase]
            axes = tuple(a for a in range(3) if a not in order[:phase])
            tail = (half, ALL, pl.ds(lane, width))
            for offset in (1, 2, 3):
                where = at_axis(axes, axis, self.torus.coord(axis, offset))
                rest = (ALL,) * (len(axes) - 1)
                self.start(self.copy(
                    self.src[phase].at[(m,) + where + tail], self.got[phase].at[(m, offset - 1) + rest + tail],
                    (phase, m, k, offset - 1), self.torus.peer(axis, offset)), ("rs", phase, m, k), go)

    def collect(self, phase, m):
        for k, (half, lane, width) in enumerate(PIECES):
            order = ORDERS[COLOURS[m][k]]
            axis = order[phase]
            axes = tuple(a for a in range(3) if a not in order[:phase])
            tail = (half, ALL, slice(lane, lane + width))
            rest = (ALL,) * (len(axes) - 1)
            self.arrive(("rs", phase, m, k))
            got = self.got[phase]
            total = self.src[phase][(m,) + at_axis(axes, axis, self.torus.coords[axis]) + tail]
            for other in range(3):
                total = total + got[(m, other) + rest + tail]
            if phase < 2:
                self.src[phase + 1][(m,) + rest + tail] = total
            else:
                self.red[m, 8 * half:8 * half + 8, lane:lane + width] = total

    def update(self, m, moment, variance):
        z, y, x = self.torus.coords
        new_mom, new_var, direction = adam_shard(moment, variance, self.red[m])
        self.gath[m, z, y, x, self.torus.core] = direction
        return new_mom, new_var

    def spread(self, phase, m):
        for j in range(2):
            order = ORDERS[UNITS[m][j]][::-1]
            axis = order[phase]
            where = tuple(ALL if a in order[:phase] else self.torus.coords[a] for a in range(3))
            ref = self.gath.at[(m,) + where + (self.torus.core, ALL, pl.ds(128 * j, 128))]
            for offset in (1, 2, 3):
                self.start(remote(
                    ref, ref, self.ag_send.at[phase, m, j, offset - 1], self.ag_recv.at[phase, m, j, offset - 1],
                    self.torus.peer(axis, offset)), ("ag", phase, m))

    def spread_arrive(self, phase, m):
        self.arrive(("ag", phase, m))

    def swap(self, m):
        self.spread_arrive(2, m)
        ref = self.gath.at[m, :, :, :, self.torus.core]
        self.start(remote(ref, ref, self.swap_send.at[m], self.swap_recv.at[m], self.torus.partner), ("swap", m))

    def finish(self):
        for cp in self.pending:
            cp.wait_send()
        self.pending = []


def step_kernel(x_hbm, dh_hbm, wu_hbm, wd_hbm, pu_hbm, pd_hbm, mom_up, var_up, mom_down, var_down,
                dir_out, state_out, gp_hbm,
                h, g, wu, wd, pu, pd, act, dz, ut0, gp, tile, tiles,
                own, pair, rb1, part1, rb2, part2, rb3, red, gath, fresh,
                in_sem, gp_sem, out_sem, state_sem, pair_send, pair_recv, rs_send, rs_recv, ag_send, ag_recv,
                swap_send, swap_recv):
    torus = Torus()
    net = Reducer(torus, tiles, own, pair, rb1, part1, rb2, part2, rb3, red, gath,
                  (pair_send, pair_recv, rs_send, rs_recv, ag_send, ag_recv, swap_send, swap_recv))
    state = ((mom_up, var_up), (mom_down, var_down))

    outs = []

    def result(m):
        net.arrive(("swap", m))
        cp = pltpu.make_async_copy(gath.at[m], dir_out.at[m], out_sem.at[m])
        cp.start()
        outs.append(cp)

    def update(m):
        net.collect(2, m)
        mom, var = state[m % 2]
        fresh[m, 0], fresh[m, 1] = net.update(m, mom[m // 2], var[m // 2])
        net.spread(0, m)
        cp = pltpu.make_async_copy(fresh.at[m], state_out.at[m], state_sem.at[m])
        cp.start()
        outs.append(cp)

    moves = {
        "begin": net.begin, "all": net.begin_all, "line": lambda m: net.step(0, m), "plane": lambda m: net.step(1, m), "adam": update,
        "pass": lambda m: net.pass_on(0, m), "fan": lambda m: net.pass_on(1, m), "swap": net.swap, "out": result,
    }

    def play(names):
        for name in names.split():
            with jax.named_scope(name):
                moves[name[:-1]](int(name[-1]))

    def run(name, body, start, stop):
        with jax.named_scope(name):
            lax.fori_loop(start, stop, body, 0)

    ut1, vt = wu.at[0, 0:256], wu.at[0, 256:512]
    loads = {}

    def load(name, src, dst):
        cp = pltpu.make_async_copy(src, dst, in_sem.at[len(loads)])
        cp.start()
        loads[name] = cp

    first, others = pl.ds(0, BLOCK), pl.ds(BLOCK, ROWS - BLOCK)
    load("x", x_hbm.at[first], h.at[first])
    load("wu0", wu_hbm.at[0], wu.at[0])
    load("pu", pu_hbm, pu)
    load("wd0", wd_hbm.at[0], wd.at[0])
    load("xs", x_hbm.at[others], h.at[others])
    load("dh", dh_hbm, g)
    load("pd", pd_hbm, pd)
    load("wu1", wu_hbm.at[1], wu.at[1])
    load("wd1", wd_hbm.at[1], wd.at[1])
    peers_ready = entry_barrier(torus)

    def slope_out(rb, half):
        part = pl.ds(2 * half, 2)
        return pltpu.make_async_copy(own.at[part], gp_hbm.at[rb, part], gp_sem.at[half])

    def slope_in(n, half):
        return pltpu.make_async_copy(gp_hbm.at[:, n // 2, pl.ds(2 * lax.rem(n, 2), 2)], gp.at[half], gp_sem.at[half])

    for name in ("x", "wu0"):
        loads[name].wait()

    def forward_zero(rb, _):
        rows = block_rows(rb)
        for half in range(2):
            @pl.when(rb > 0)
            def _():
                slope_out(rb - 1, half).wait()

            for n in range(4 * half, 4 * half + 4):
                cols = slice(TILE * n, TILE * n + TILE)
                value, slope = gelu_pair(dot(h[rows], wu[0, :, cols]))
                act[rows, cols] = value.astype(BF16)
                own[n // 2, 2 * (n % 2):2 * (n % 2) + 2] = slope.reshape(PIECE)
            slope_out(rb, half).start()

        @pl.when(rb == 0)
        def _():
            loads["wd0"].wait()
            loads["xs"].wait()
            loads["pu"].wait()

        ut0[:, rows] = dot(h[rows], pu[0]).astype(BF16).T
        for k in range(3):
            cols = slice(256 * k, 256 * k + 256)
            h[rows, cols] = (h[rows, cols] + dot(act[rows], wd[0, :, cols])).astype(BF16)
        return 0

    run("fwd0", forward_zero, 0, BLOCKS)
    for name in ("dh", "pd", "wu1", "wd1"):
        loads[name].wait()
    for half in range(2):
        slope_out(BLOCKS - 1, half).wait()

    def project_one(rb, _):
        rows = block_rows(rb)
        ut1[:, rows] = dot(h[rows], pu[1]).astype(BF16).T
        vt[:, rows] = dot(g[rows], pd[1]).astype(BF16).T
        return 0

    run("proj1", project_one, 0, BLOCKS)

    def layer_one(n, _):
        cols = tile_cols(n)
        slot = 2 * lax.rem(n, 2)

        @pl.when(n >= 2)
        def _():
            net.pair_copy(3, n - 2, slot).wait_send()
            net.pair_copy(2, n - 2, slot + 1).wait_send()

        @pl.when((n >= 3) & (lax.rem(n, 2) == 1))
        def _():
            net.slab(3, n // 2 - 1)
            net.slab(2, n // 2 - 1)

        for rc in range(BLOCKS):
            rows = slice(BLOCK * rc, BLOCK * rc + BLOCK)
            value, slope = gelu_pair(dot(h[rows], wu[1, :, cols]))
            tile[rows] = value.astype(BF16)
            dz[rows, cols] = (slope * dot_t(g[rows], wd[1, cols, :])).astype(BF16)
        net.emit(3, n, slot, dot(vt[...], tile[...]))
        net.emit(2, n, slot + 1, dot(ut1[...], dz[:, cols]))
        return 0

    peers_ready()
    run("layer1", layer_one, 0, TILES)

    def input_grad(rb, _):
        rows = block_rows(rb)
        for k in range(3):
            cols = slice(256 * k, 256 * k + 256)
            g[rows, cols] = (g[rows, cols] + dot_t(dz[rows], wu[1, cols, :])).astype(BF16)
        vt[:, rows] = dot(g[rows], pd[0]).astype(BF16).T
        return 0

    run("g1a", input_grad, 0, 1)
    play("begin3 begin2")
    run("g1b", input_grad, 1, BLOCKS)
    play("line3 line2")
    for n in (TILES - 2, TILES - 1):
        net.pair_copy(3, n, 2 * (n % 2)).wait_send()
        net.pair_copy(2, n, 2 * (n % 2) + 1).wait_send()

    def down_zero(n, _):
        slot = lax.rem(n, 4)

        @pl.when(n >= 4)
        def _():
            net.pair_copy(1, n - 4, slot).wait_send()

        net.emit(1, n, slot, dot(vt[...], act[:, tile_cols(n)]))
        return 0

    slope_in(0, 0).start()
    run("down0", down_zero, 0, TILES)
    for n in range(4, TILES):
        net.pair_copy(1, n, n % 4).wait_send()

    def up_rows(n):
        half = lax.rem(n, 2)
        slope_in(n, half).wait()

        @pl.when(n < TILES - 1)
        def _():
            slope_in(n + 1, 1 - half).start()

        for rc in range(BLOCKS):
            rows = slice(BLOCK * rc, BLOCK * rc + BLOCK)
            d_act = dot_t(g[rows], wd[0, tile_cols(n), :])
            h[rows, tile_cols(half)] = (gp[half, rc].reshape(BLOCK, TILE) * d_act).astype(BF16)

    def up_sum(n):
        net.emit(0, n, lax.rem(n, 4), dot(ut0[...], h[:, tile_cols(lax.rem(n, 2))]))

    def up_zero(n, _):
        @pl.when(n >= 5)
        def _():
            net.pair_copy(0, n - 5, lax.rem(n - 1, 4)).wait_send()

        @pl.when((n >= 4) & (lax.rem(n, 2) == 0))
        def _():
            net.slab(0, n // 2 - 2)

        up_rows(n)
        up_sum(n - 1)
        return 0

    play("plane3 plane2 all1")
    up_rows(0)
    first = 1
    for last, names in SCHEDULE:
        run(f"up{first}", up_zero, first, last)
        play(names)
        first = last
    net.pair_copy(0, 3, 3).wait_send()
    up_sum(TILES - 1)
    net.slab(0, 2)
    for names in LAST:
        play(names)
    for names in TAIL:
        play(names)
    for n in range(4, TILES):
        net.pair_copy(0, n, n % 4).wait_send()
    net.finish()
    play("swap0 out1 out0")
    net.finish()
    for cp in outs:
        cp.wait()


def train_step(x_rows, dh_rows, w_up, w_down, proj_up, proj_down, moments):
    hbm = pl.BlockSpec(memory_space=pl.ANY)
    vmem = pl.BlockSpec(memory_space=pltpu.VMEM)
    dma = pltpu.SemaphoreType.DMA

    def sums(lines, *lead):
        return pltpu.VMEM(lead + (4,) * lines + (2, 8, RANK), F32)

    return pl.pallas_call(
        step_kernel,
        out_shape=(jax.ShapeDtypeStruct(DIRECTIONS, BF16), jax.ShapeDtypeStruct((4, 2, 16, RANK), F32),
                   jax.ShapeDtypeStruct((BLOCKS, 4) + (4,) * 3 + (2, 8, RANK), F32)),
        in_specs=[hbm] * 6 + [vmem] * 4,
        out_specs=(hbm,) * 3,
        scratch_shapes=[
            pltpu.VMEM((ROWS, WIDTH), BF16),
            pltpu.VMEM((ROWS, WIDTH), BF16),
            pltpu.VMEM(w_up.shape, BF16),
            pltpu.VMEM(w_down.shape, BF16),
            pltpu.VMEM(proj_up.shape, BF16),
            pltpu.VMEM(proj_down.shape, BF16),
            pltpu.VMEM((ROWS, FF), BF16),
            pltpu.VMEM((ROWS, FF), BF16),
            pltpu.VMEM((RANK, ROWS), BF16),
            pltpu.VMEM((2, BLOCKS) + PIECE, F32),
            pltpu.VMEM((ROWS, TILE), BF16),
            pltpu.VMEM((4, 2, 4, 2, 2, 8, RANK), F32),
            sums(3, 4), sums(3, 4),
            sums(2, 4, 3), sums(2, 4),
            sums(1, 4, 3), sums(1, 4),
            sums(0, 4, 3),
            pltpu.VMEM((4, 16, RANK), F32),
            pltpu.VMEM(DIRECTIONS, BF16),
            pltpu.VMEM((4, 2, 16, RANK), F32),
            dma((9,)), dma((2,)), dma((4,)), dma((4,)), dma((4,)), dma((4, TILES)),
            dma((3, 4, 3, 3)), dma((3, 4, 3, 3)),
            dma((3, 4, 2, 3)), dma((3, 4, 2, 3)),
            dma((4,)), dma((4,)),
        ],
        compiler_params=pltpu.CompilerParams(
            collective_id=0, has_side_effects=True, vmem_limit_bytes=67_043_328),
    )(x_rows, dh_rows, w_up, w_down, proj_up, proj_down, *moments)


def weight_kernel(dirs, w_up, w_down, proj_up, proj_down, state, new_up, new_down, mom_up, var_up, mom_down, var_down,
                  n_buf, up_buf, down_buf, pu, pd, s_buf, in_sem, small_sem, out_sem, state_sem):
    def chunk(q):
        return q // 4, pl.ds(pl.multiple_of(BLOCK * lax.rem(q, 4), BLOCK), BLOCK)

    def inputs(q):
        l, part = chunk(q)
        pairs = (
            (dirs.at[2 * l, part], n_buf.at[0, l, part]), (dirs.at[2 * l + 1, part], n_buf.at[1, l, part]),
            (w_up.at[l, ALL, part], up_buf.at[l, ALL, part]), (w_down.at[l, part], down_buf.at[l, part]),
        )
        return [pltpu.make_async_copy(src, dst, in_sem.at[k, q]) for k, (src, dst) in enumerate(pairs)]

    def outputs(q):
        l, part = chunk(q)
        pairs = ((up_buf.at[l, ALL, part], new_up.at[l, ALL, part]), (down_buf.at[l, part], new_down.at[l, part]))
        return [pltpu.make_async_copy(src, dst, out_sem.at[k, q]) for k, (src, dst) in enumerate(pairs)]

    def each(copies, action):
        def body(q, _):
            for cp in copies(q):
                action(cp)
            return 0

        lax.fori_loop(0, TILES, body, 0)

    smalls = [pltpu.make_async_copy(src, dst, small_sem.at[k])
              for k, (src, dst) in enumerate(((proj_up, pu), (proj_down, pd), (state, s_buf)))]
    for cp in smalls:
        cp.start()
    each(inputs, lambda cp: cp.start())
    for cp in smalls:
        cp.wait()
    leaving = []
    for m in range(4):
        for k, dst in enumerate(((mom_up, var_up), (mom_down, var_down))[m % 2]):
            leaving.append(pltpu.make_async_copy(s_buf.at[m, k], dst.at[m // 2], state_sem.at[m, k]))
            leaving[-1].start()

    def compute(q, _):
        l, part = chunk(q)
        for cp in inputs(q):
            cp.wait()
        up_buf[l, :, part] = (up_buf[l, :, part] - SCALE * dot_t(pu[l], n_buf[0, l, part])).astype(BF16)
        down_buf[l, part] = (down_buf[l, part] - SCALE * dot_t(n_buf[1, l, part], pd[l])).astype(BF16)
        for cp in outputs(q):
            cp.start()
        return 0

    lax.fori_loop(0, TILES, compute, 0)
    each(outputs, lambda cp: cp.wait())
    for cp in leaving:
        cp.wait()


def new_weights(directions, w_up, w_down, proj_up, proj_down, state):
    hbm = pl.BlockSpec(memory_space=pl.ANY)
    dma = pltpu.SemaphoreType.DMA
    return pl.pallas_call(
        weight_kernel,
        out_shape=(jax.ShapeDtypeStruct(w_up.shape, BF16), jax.ShapeDtypeStruct(w_down.shape, BF16))
        + (jax.ShapeDtypeStruct((2, 16, RANK), F32),) * 4,
        in_specs=[hbm] * 6,
        out_specs=(hbm,) * 6,
        scratch_shapes=[
            pltpu.VMEM((2, 2, FF, RANK), BF16),
            pltpu.VMEM(w_up.shape, BF16),
            pltpu.VMEM(w_down.shape, BF16),
            pltpu.VMEM(proj_up.shape, BF16),
            pltpu.VMEM(proj_down.shape, BF16),
            pltpu.VMEM(state.shape, F32),
            dma((4, TILES)), dma((3,)), dma((2, TILES)), dma((4, 2)),
        ],
    )(directions, w_up, w_down, proj_up, proj_down, state)


def solution(mesh):
    def local_step(x_loc, dh_loc, w_up, w_down, proj_up, proj_down, mom_up, var_up, mom_down, var_down):
        moments = (jnp.swapaxes(mom_up, 1, 2), jnp.swapaxes(var_up, 1, 2), mom_down, var_down)
        directions, state, _ = train_step(x_loc, dh_loc, w_up, w_down, proj_up, proj_down, moments)
        new_up, new_down, *moments = new_weights(
            directions.reshape(4, 2048, 256), w_up, w_down, proj_up, proj_down, state)
        return (new_up, new_down, jnp.swapaxes(moments[0], 1, 2), jnp.swapaxes(moments[1], 1, 2), moments[2], moments[3])

    tok_spec = P('data', None)
    up_spec = P(None, None, 'data')
    down_spec = P(None, 'data', None)
    return jax.shard_map(
        local_step,
        mesh=mesh,
        in_specs=(tok_spec, tok_spec, P(), P(), P(), P(), up_spec, up_spec, down_spec, down_spec),
        out_specs=(P(), P(), up_spec, up_spec, down_spec, down_spec),
        check_vma=False,
    )
```

```python
import jax
import jax.numpy as jnp
from jax import lax
from jax.experimental import pallas as pl
from jax.experimental.pallas import tpu as pltpu
from jax.sharding import PartitionSpec as P

BETA_ONE = 0.9
BETA_TWO = 0.999
EPSILON = 1e-8
STEP = 4
LEARN_RATE = 0.02
ALPHA_SCALE = 0.25
SCALE = LEARN_RATE * ALPHA_SCALE
GELU_A = 0.7978845608028654
GELU_B = 0.044715
MESH = pl.DeviceIdType.MESH
ALL = slice(None)
ROWS, WIDTH, FF, RANK = 2048, 768, 2048, 256
F32, BF16 = jnp.float32, jnp.bfloat16

PIECE = (2, 4, 4, 2, 8, RANK)
DIRECTIONS = (4,) * 4 + (2, 16, RANK)
BLOCK = 512
TILE = 256
BLOCKS = 4
TILES = 8

ORDERS = ((2, 1, 0), (1, 0, 2), (0, 2, 1))
COLOURS = ((0, 1, 2), (1, 2, 0), (2, 0, 1), (0, 1, 2))
PIECES = ((0, 0, 256), (1, 0, 128), (1, 128, 128))
UNITS = ((0, 1), (2, 0), (1, 2), (0, 1))
SCHEDULE = (
    (2, "adam3 adam2"),
    (4, "pass3 pass2"),
    (6, "line1 fan3 fan2"),
    (8, "plane1"),
)
LAST = ("begin0 swap3 swap2 adam1",)
TAIL = ("line0 pass1 plane0 fan1", "adam0 pass0 out3 out2", "fan0 swap1")


def dot(lhs, rhs):
    return jnp.dot(lhs, rhs, preferred_element_type=F32)


def dot_t(lhs, rhs):
    return lax.dot_general(lhs, rhs, (((1,), (1,)), ((), ())), preferred_element_type=F32)


def gelu_pair(z):
    sq = z * z
    cdf = 0.5 + 0.5 * jnp.tanh(z * (GELU_A + (GELU_A * GELU_B) * sq))
    act = z * cdf
    slope = cdf + act * ((1.0 - cdf) * (2.0 * GELU_A + (6.0 * GELU_A * GELU_B) * sq))
    return act, slope


def adam_shard(moment, variance, grad_red):
    new_mom = BETA_ONE * moment + (1.0 - BETA_ONE) * grad_red
    new_var = BETA_TWO * variance + (1.0 - BETA_TWO) * grad_red * grad_red
    bias_one = 1.0 - BETA_ONE ** STEP
    bias_two = 1.0 - BETA_TWO ** STEP
    direction = (new_mom / bias_one) / (jnp.sqrt(new_var / bias_two) + EPSILON)
    return new_mom, new_var, direction.astype(BF16)


def block_rows(i):
    return pl.ds(pl.multiple_of(i * BLOCK, BLOCK), BLOCK)


def tile_cols(n):
    return pl.ds(pl.multiple_of(n * TILE, TILE), TILE)


class Torus:
    def __init__(self):
        me = lax.axis_index("data")
        self.core = lax.rem(me, 2)
        chip = me // 2
        self.coords = (chip // 16, lax.rem(chip // 4, 4), lax.rem(chip, 4))
        self.partner = me + 1 - 2 * self.core

    def coord(self, axis, offset):
        return lax.rem(self.coords[axis] + offset, 4)

    def peer(self, axis, offset):
        z, y, x = (self.coord(a, offset) if a == axis else self.coords[a] for a in range(3))
        return ((z * 4 + y) * 4 + x) * 2 + self.core


def remote(src, dst, send_sem, recv_sem, device):
    return pltpu.make_async_remote_copy(
        src_ref=src, dst_ref=dst, send_sem=send_sem, recv_sem=recv_sem,
        device_id=(device,), device_id_type=MESH,
    )


def entry_barrier(torus):
    barrier = pltpu.get_barrier_semaphore()
    pl.semaphore_signal(barrier, inc=1, device_id=(torus.partner,), device_id_type=MESH)
    for axis in range(3):
        for offset in (1, 2, 3):
            pl.semaphore_signal(barrier, inc=1, device_id=(torus.peer(axis, offset),), device_id_type=MESH)
    return lambda: pl.semaphore_wait(barrier, 10)


def at_axis(axes, axis, index):
    return tuple(index if a == axis else ALL for a in axes)


class Reducer:
    def __init__(self, torus, tiles, own, pair, rb1, part1, rb2, part2, rb3, red, gath, sems):
        self.torus = torus
        self.tiles = tiles
        self.src = (own, part1, part2)
        self.got = (rb1, rb2, rb3)
        self.pair, self.red, self.gath = pair, red, gath
        (self.pair_send, self.pair_recv, self.rs_send, self.rs_recv, self.ag_send, self.ag_recv, self.swap_send,
         self.swap_recv) = sems
        self.pending = []
        self.inbound = {}

    def pair_copy(self, m, n, slot):
        where = (m, n // 2, pl.ds(2 * lax.rem(n, 2), 2))
        return remote(self.tiles.at[slot, :, :, 1 - self.torus.core], self.pair.at[where],
                      self.pair_send.at[slot], self.pair_recv.at[m, n], self.torus.partner)

    def emit(self, m, n, slot, part):
        self.tiles[slot] = part.T.reshape(2, 4, 2, 2, 8, 256)
        self.src[0][m, n // 2, pl.ds(2 * lax.rem(n, 2), 2)] = self.tiles[slot, :, :, self.torus.core]
        self.pair_copy(m, n, slot).start()

    def slab(self, m, z):
        own, pair = self.src[0], self.pair
        for half in range(2):
            self.pair_copy(m, 2 * z + half, 0).wait_recv()
        own[m, z] = own[m, z] + pair[m, z]
        for k, (half, lane, width) in enumerate(PIECES):
            axis = ORDERS[COLOURS[m][k]][0]
            tail = (half, ALL, pl.ds(lane, width))
            if axis == 0:
                offset = lax.rem(z + 4 - self.torus.coords[0], 4)

                @pl.when(offset > 0)
                def _():
                    self.copy(own.at[(m, z) + (ALL,) * 2 + tail],
                              self.got[0].at[(m, offset - 1) + (ALL,) * 2 + tail],
                              (0, m, k, offset - 1), self.torus.peer(0, offset)).start()
                continue
            for offset in (1, 2, 3):
                where = at_axis((1, 2), axis, self.torus.coord(axis, offset))
                self.copy(own.at[(m, z) + where + tail], self.got[0].at[(m, offset - 1, z, ALL) + tail],
                          (0, m, k, offset - 1), self.torus.peer(axis, offset)).start()

    def begin(self, m):
        self.slab(m, 3)
        self.scatter(0, m, False)

    def begin_all(self, m):
        lax.fori_loop(0, 3, lambda z, _: (self.slab(m, z), 0)[1], 0)
        self.begin(m)

    def copy(self, src, dst, sem, device):
        return remote(src, dst, self.rs_send.at[sem], self.rs_recv.at[sem], device)

    def step(self, phase, m):
        self.collect(phase, m)
        self.scatter(phase + 1, m)

    def pass_on(self, phase, m):
        self.spread_arrive(phase, m)
        self.spread(phase + 1, m)

    def start(self, cp, key, go=True):
        if go:
            cp.start()
        self.pending.append(cp)
        self.inbound.setdefault(key, []).append(cp)

    def arrive(self, key):
        for cp in self.inbound[key]:
            cp.wait_recv()

    def scatter(self, phase, m, go=True):
        for k, (half, lane, width) in enumerate(PIECES):
            order = ORDERS[COLOURS[m][k]]
            axis = order[phase]
            axes = tuple(a for a in range(3) if a not in order[:phase])
            tail = (half, ALL, pl.ds(lane, width))
            for offset in (1, 2, 3):
                where = at_axis(axes, axis, self.torus.coord(axis, offset))
                rest = (ALL,) * (len(axes) - 1)
                self.start(self.copy(
                    self.src[phase].at[(m,) + where + tail], self.got[phase].at[(m, offset - 1) + rest + tail],
                    (phase, m, k, offset - 1), self.torus.peer(axis, offset)), ("rs", phase, m, k), go)

    def collect(self, phase, m):
        for k, (half, lane, width) in enumerate(PIECES):
            order = ORDERS[COLOURS[m][k]]
            axis = order[phase]
            axes = tuple(a for a in range(3) if a not in order[:phase])
            tail = (half, ALL, slice(lane, lane + width))
            rest = (ALL,) * (len(axes) - 1)
            self.arrive(("rs", phase, m, k))
            got = self.got[phase]
            total = self.src[phase][(m,) + at_axis(axes, axis, self.torus.coords[axis]) + tail]
            for other in range(3):
                total = total + got[(m, other) + rest + tail]
            if phase < 2:
                self.src[phase + 1][(m,) + rest + tail] = total
            else:
                self.red[m, 8 * half:8 * half + 8, lane:lane + width] = total

    def update(self, m, moment, variance):
        z, y, x = self.torus.coords
        new_mom, new_var, direction = adam_shard(moment, variance, self.red[m])
        self.gath[m, z, y, x, self.torus.core] = direction
        return new_mom, new_var

    def spread(self, phase, m):
        for j in range(2):
            order = ORDERS[UNITS[m][j]][::-1]
            axis = order[phase]
            where = tuple(ALL if a in order[:phase] else self.torus.coords[a] for a in range(3))
            ref = self.gath.at[(m,) + where + (self.torus.core, ALL, pl.ds(128 * j, 128))]
            for offset in (1, 2, 3):
                self.start(remote(
                    ref, ref, self.ag_send.at[phase, m, j, offset - 1], self.ag_recv.at[phase, m, j, offset - 1],
                    self.torus.peer(axis, offset)), ("ag", phase, m))

    def spread_arrive(self, phase, m):
        self.arrive(("ag", phase, m))

    def swap(self, m):
        self.spread_arrive(2, m)
        ref = self.gath.at[m, :, :, :, self.torus.core]
        self.start(remote(ref, ref, self.swap_send.at[m], self.swap_recv.at[m], self.torus.partner), ("swap", m))

    def finish(self):
        for cp in self.pending:
            cp.wait_send()
        self.pending = []


def step_kernel(x_hbm, dh_hbm, wu_hbm, wd_hbm, pu_hbm, pd_hbm, mom_up, var_up, mom_down, var_down,
                dir_out, state_out, gp_hbm,
                h, g, wu, wd, pu, pd, act, dz, ut0, gp, tile, parts, tiles,
                own, pair, rb1, part1, rb2, part2, rb3, red, gath, fresh,
                in_sem, gp_sem, out_sem, state_sem, pair_send, pair_recv, rs_send, rs_recv, ag_send, ag_recv,
                swap_send, swap_recv):
    torus = Torus()
    net = Reducer(torus, tiles, own, pair, rb1, part1, rb2, part2, rb3, red, gath,
                  (pair_send, pair_recv, rs_send, rs_recv, ag_send, ag_recv, swap_send, swap_recv))
    state = ((mom_up, var_up), (mom_down, var_down))

    outs = []

    def result(m):
        net.arrive(("swap", m))
        cp = pltpu.make_async_copy(gath.at[m], dir_out.at[m], out_sem.at[m])
        cp.start()
        outs.append(cp)

    def update(m):
        net.collect(2, m)
        mom, var = state[m % 2]
        fresh[m, 0], fresh[m, 1] = net.update(m, mom[m // 2], var[m // 2])
        net.spread(0, m)
        cp = pltpu.make_async_copy(fresh.at[m], state_out.at[m], state_sem.at[m])
        cp.start()
        outs.append(cp)

    moves = {
        "begin": net.begin, "all": net.begin_all, "line": lambda m: net.step(0, m), "plane": lambda m: net.step(1, m), "adam": update,
        "pass": lambda m: net.pass_on(0, m), "fan": lambda m: net.pass_on(1, m), "swap": net.swap, "out": result,
    }

    def play(names):
        for name in names.split():
            with jax.named_scope(name):
                moves[name[:-1]](int(name[-1]))

    def run(name, body, start, stop):
        with jax.named_scope(name):
            lax.fori_loop(start, stop, body, 0)

    ut1, vt = wu.at[0, 0:256], wu.at[0, 256:512]
    loads = {}

    def load(name, src, dst):
        cp = pltpu.make_async_copy(src, dst, in_sem.at[len(loads)])
        cp.start()
        loads[name] = cp

    first, others = pl.ds(0, BLOCK), pl.ds(BLOCK, ROWS - BLOCK)
    load("x", x_hbm.at[first], h.at[first])
    load("wu0", wu_hbm.at[0], wu.at[0])
    load("pu", pu_hbm, pu)
    load("wd0", wd_hbm.at[0], wd.at[0])
    load("xs", x_hbm.at[others], h.at[others])
    load("dh", dh_hbm, g)
    load("pd", pd_hbm, pd)
    load("wu1", wu_hbm.at[1], wu.at[1])
    load("wd1", wd_hbm.at[1], wd.at[1])
    peers_ready = entry_barrier(torus)

    def slope_out(rb, half):
        part = pl.ds(2 * half, 2)
        return pltpu.make_async_copy(own.at[part], gp_hbm.at[rb, part], gp_sem.at[half])

    def slope_in(n, half):
        return pltpu.make_async_copy(gp_hbm.at[:, n // 2, pl.ds(2 * lax.rem(n, 2), 2)], gp.at[half], gp_sem.at[half])

    for name in ("x", "wu0"):
        loads[name].wait()

    def forward_zero(rb, _):
        rows = block_rows(rb)
        for half in range(2):
            @pl.when(rb > 0)
            def _():
                slope_out(rb - 1, half).wait()

            for n in range(4 * half, 4 * half + 4):
                cols = slice(TILE * n, TILE * n + TILE)
                value, slope = gelu_pair(dot(h[rows], wu[0, :, cols]))
                act[rows, cols] = value.astype(BF16)
                own[n // 2, 2 * (n % 2):2 * (n % 2) + 2] = slope.reshape(PIECE)
            slope_out(rb, half).start()

        @pl.when(rb == 0)
        def _():
            loads["wd0"].wait()
            loads["xs"].wait()
            loads["pu"].wait()

        ut0[:, rows] = dot(h[rows], pu[0]).astype(BF16).T
        for k in range(3):
            cols = slice(256 * k, 256 * k + 256)
            h[rows, cols] = (h[rows, cols] + dot(act[rows], wd[0, :, cols])).astype(BF16)
        return 0

    run("fwd0", forward_zero, 0, BLOCKS)
    for name in ("dh", "pd", "wu1", "wd1"):
        loads[name].wait()
    for half in range(2):
        slope_out(BLOCKS - 1, half).wait()

    def project_one(rb, _):
        rows = block_rows(rb)
        ut1[:, rows] = dot(h[rows], pu[1]).astype(BF16).T
        vt[:, rows] = dot(g[rows], pd[1]).astype(BF16).T
        return 0

    run("proj1", project_one, 0, BLOCKS)

    def layer_rows(n):
        cols = tile_cols(n)
        for rc in range(BLOCKS):
            rows = slice(BLOCK * rc, BLOCK * rc + BLOCK)
            value, slope = gelu_pair(dot(h[rows], wu[1, :, cols]))
            tile[rows] = value.astype(BF16)
            dz[rows, cols] = (slope * dot_t(g[rows], wd[1, cols, :])).astype(BF16)
        parts[0] = dot(vt[...], tile[...])
        parts[1] = dot(ut1[...], dz[:, cols])

    def layer_emit(n):
        slot = 2 * lax.rem(n, 2)
        net.emit(3, n, slot, parts[0])
        net.emit(2, n, slot + 1, parts[1])

    def layer_free(n):
        slot = 2 * lax.rem(n, 2)
        net.pair_copy(3, n - 2, slot).wait_send()
        net.pair_copy(2, n - 2, slot + 1).wait_send()

    def layer_one(n, _):
        @pl.when(n >= 3)
        def _():
            layer_free(n - 1)

        @pl.when((n >= 4) & (lax.rem(n, 2) == 0))
        def _():
            net.slab(3, n // 2 - 2)
            net.slab(2, n // 2 - 2)

        layer_emit(n - 1)
        layer_rows(n)
        return 0

    peers_ready()
    layer_rows(0)
    run("layer1", layer_one, 1, TILES)
    layer_free(TILES - 1)
    layer_emit(TILES - 1)
    net.slab(3, 2)
    net.slab(2, 2)

    def input_grad(rb, _):
        rows = block_rows(rb)
        for k in range(3):
            cols = slice(256 * k, 256 * k + 256)
            g[rows, cols] = (g[rows, cols] + dot_t(dz[rows], wu[1, cols, :])).astype(BF16)
        vt[:, rows] = dot(g[rows], pd[0]).astype(BF16).T
        return 0

    run("g1a", input_grad, 0, 1)
    play("begin3 begin2")
    run("g1b", input_grad, 1, BLOCKS)
    play("line3 line2")
    for n in (TILES - 2, TILES - 1):
        net.pair_copy(3, n, 2 * (n % 2)).wait_send()
        net.pair_copy(2, n, 2 * (n % 2) + 1).wait_send()

    def down_zero(pair, _):
        @pl.when(pair >= 2)
        def _():
            for k in range(2):
                n = 2 * pair + k
                net.pair_copy(1, n - 4, lax.rem(n, 4)).wait_send()

        for k in range(2):
            n = 2 * pair + k
            net.emit(1, n, lax.rem(n, 4), dot(vt[...], act[:, tile_cols(n)]))
        return 0

    slope_in(0, 0).start()
    run("down0", down_zero, 0, TILES // 2)
    for n in range(4, TILES):
        net.pair_copy(1, n, n % 4).wait_send()

    def up_rows(n):
        half = lax.rem(n, 2)
        slope_in(n, half).wait()

        @pl.when(n < TILES - 1)
        def _():
            slope_in(n + 1, 1 - half).start()

        for rc in range(BLOCKS):
            rows = slice(BLOCK * rc, BLOCK * rc + BLOCK)
            d_act = dot_t(g[rows], wd[0, tile_cols(n), :])
            h[rows, tile_cols(half)] = (gp[half, rc].reshape(BLOCK, TILE) * d_act).astype(BF16)

    def up_sum(n):
        net.emit(0, n, lax.rem(n, 4), dot(ut0[...], h[:, tile_cols(lax.rem(n, 2))]))

    def up_zero(n, _):
        @pl.when(n >= 5)
        def _():
            net.pair_copy(0, n - 5, lax.rem(n - 1, 4)).wait_send()

        @pl.when((n >= 4) & (lax.rem(n, 2) == 0))
        def _():
            net.slab(0, n // 2 - 2)

        up_rows(n)
        up_sum(n - 1)
        return 0

    play("plane3 plane2 all1")
    up_rows(0)
    first = 1
    for last, names in SCHEDULE:
        run(f"up{first}", up_zero, first, last)
        play(names)
        first = last
    net.pair_copy(0, 3, 3).wait_send()
    up_sum(TILES - 1)
    net.slab(0, 2)
    for names in LAST:
        play(names)
    for names in TAIL:
        play(names)
    for n in range(4, TILES):
        net.pair_copy(0, n, n % 4).wait_send()
    net.finish()
    play("swap0 out1 out0")
    net.finish()
    for cp in outs:
        cp.wait()


def train_step(x_rows, dh_rows, w_up, w_down, proj_up, proj_down, moments):
    hbm = pl.BlockSpec(memory_space=pl.ANY)
    vmem = pl.BlockSpec(memory_space=pltpu.VMEM)
    dma = pltpu.SemaphoreType.DMA

    def sums(lines, *lead):
        return pltpu.VMEM(lead + (4,) * lines + (2, 8, RANK), F32)

    return pl.pallas_call(
        step_kernel,
        out_shape=(jax.ShapeDtypeStruct(DIRECTIONS, BF16), jax.ShapeDtypeStruct((4, 2, 16, RANK), F32),
                   jax.ShapeDtypeStruct((BLOCKS, 4) + (4,) * 3 + (2, 8, RANK), F32)),
        in_specs=[hbm] * 6 + [vmem] * 4,
        out_specs=(hbm,) * 3,
        scratch_shapes=[
            pltpu.VMEM((ROWS, WIDTH), BF16),
            pltpu.VMEM((ROWS, WIDTH), BF16),
            pltpu.VMEM(w_up.shape, BF16),
            pltpu.VMEM(w_down.shape, BF16),
            pltpu.VMEM(proj_up.shape, BF16),
            pltpu.VMEM(proj_down.shape, BF16),
            pltpu.VMEM((ROWS, FF), BF16),
            pltpu.VMEM((ROWS, FF), BF16),
            pltpu.VMEM((RANK, ROWS), BF16),
            pltpu.VMEM((2, BLOCKS) + PIECE, F32),
            pltpu.VMEM((ROWS, TILE), BF16),
            pltpu.VMEM((2, RANK, TILE), F32),
            pltpu.VMEM((4, 2, 4, 2, 2, 8, RANK), F32),
            sums(3, 4), sums(3, 4),
            sums(2, 4, 3), sums(2, 4),
            sums(1, 4, 3), sums(1, 4),
            sums(0, 4, 3),
            pltpu.VMEM((4, 16, RANK), F32),
            pltpu.VMEM(DIRECTIONS, BF16),
            pltpu.VMEM((4, 2, 16, RANK), F32),
            dma((9,)), dma((2,)), dma((4,)), dma((4,)), dma((4,)), dma((4, TILES)),
            dma((3, 4, 3, 3)), dma((3, 4, 3, 3)),
            dma((3, 4, 2, 3)), dma((3, 4, 2, 3)),
            dma((4,)), dma((4,)),
        ],
        compiler_params=pltpu.CompilerParams(
            collective_id=0, has_side_effects=True, vmem_limit_bytes=67_043_328),
    )(x_rows, dh_rows, w_up, w_down, proj_up, proj_down, *moments)


def weight_kernel(dirs, w_up, w_down, proj_up, proj_down, state, new_up, new_down, mom_up, var_up, mom_down, var_down,
                  n_buf, up_buf, down_buf, pu, pd, s_buf, in_sem, small_sem, out_sem, state_sem):
    def chunk(q):
        return q // 4, pl.ds(pl.multiple_of(BLOCK * lax.rem(q, 4), BLOCK), BLOCK)

    def inputs(q):
        l, part = chunk(q)
        pairs = (
            (dirs.at[2 * l, part], n_buf.at[0, l, part]), (dirs.at[2 * l + 1, part], n_buf.at[1, l, part]),
            (w_up.at[l, ALL, part], up_buf.at[l, ALL, part]), (w_down.at[l, part], down_buf.at[l, part]),
        )
        return [pltpu.make_async_copy(src, dst, in_sem.at[k, q]) for k, (src, dst) in enumerate(pairs)]

    def outputs(q):
        l, part = chunk(q)
        pairs = ((up_buf.at[l, ALL, part], new_up.at[l, ALL, part]), (down_buf.at[l, part], new_down.at[l, part]))
        return [pltpu.make_async_copy(src, dst, out_sem.at[k, q]) for k, (src, dst) in enumerate(pairs)]

    def each(copies, action):
        def body(q, _):
            for cp in copies(q):
                action(cp)
            return 0

        lax.fori_loop(0, TILES, body, 0)

    smalls = [pltpu.make_async_copy(src, dst, small_sem.at[k])
              for k, (src, dst) in enumerate(((proj_up, pu), (proj_down, pd), (state, s_buf)))]
    for cp in smalls:
        cp.start()
    each(inputs, lambda cp: cp.start())
    for cp in smalls:
        cp.wait()
    leaving = []
    for m in range(4):
        for k, dst in enumerate(((mom_up, var_up), (mom_down, var_down))[m % 2]):
            leaving.append(pltpu.make_async_copy(s_buf.at[m, k], dst.at[m // 2], state_sem.at[m, k]))
            leaving[-1].start()

    def compute(q, _):
        l, part = chunk(q)
        for cp in inputs(q):
            cp.wait()
        up_buf[l, :, part] = (up_buf[l, :, part] - SCALE * dot_t(pu[l], n_buf[0, l, part])).astype(BF16)
        down_buf[l, part] = (down_buf[l, part] - SCALE * dot_t(n_buf[1, l, part], pd[l])).astype(BF16)
        for cp in outputs(q):
            cp.start()
        return 0

    lax.fori_loop(0, TILES, compute, 0)
    each(outputs, lambda cp: cp.wait())
    for cp in leaving:
        cp.wait()


def new_weights(directions, w_up, w_down, proj_up, proj_down, state):
    hbm = pl.BlockSpec(memory_space=pl.ANY)
    dma = pltpu.SemaphoreType.DMA
    return pl.pallas_call(
        weight_kernel,
        out_shape=(jax.ShapeDtypeStruct(w_up.shape, BF16), jax.ShapeDtypeStruct(w_down.shape, BF16))
        + (jax.ShapeDtypeStruct((2, 16, RANK), F32),) * 4,
        in_specs=[hbm] * 6,
        out_specs=(hbm,) * 6,
        scratch_shapes=[
            pltpu.VMEM((2, 2, FF, RANK), BF16),
            pltpu.VMEM(w_up.shape, BF16),
            pltpu.VMEM(w_down.shape, BF16),
            pltpu.VMEM(proj_up.shape, BF16),
            pltpu.VMEM(proj_down.shape, BF16),
            pltpu.VMEM(state.shape, F32),
            dma((4, TILES)), dma((3,)), dma((2, TILES)), dma((4, 2)),
        ],
    )(directions, w_up, w_down, proj_up, proj_down, state)


def solution(mesh):
    def local_step(x_loc, dh_loc, w_up, w_down, proj_up, proj_down, mom_up, var_up, mom_down, var_down):
        moments = (jnp.swapaxes(mom_up, 1, 2), jnp.swapaxes(var_up, 1, 2), mom_down, var_down)
        directions, state, _ = train_step(x_loc, dh_loc, w_up, w_down, proj_up, proj_down, moments)
        new_up, new_down, *moments = new_weights(
            directions.reshape(4, 2048, 256), w_up, w_down, proj_up, proj_down, state)
        return (new_up, new_down, jnp.swapaxes(moments[0], 1, 2), jnp.swapaxes(moments[1], 1, 2), moments[2], moments[3])

    tok_spec = P('data', None)
    up_spec = P(None, None, 'data')
    down_spec = P(None, 'data', None)
    return jax.shard_map(
        local_step,
        mesh=mesh,
        in_specs=(tok_spec, tok_spec, P(), P(), P(), P(), up_spec, up_spec, down_spec, down_spec),
        out_specs=(P(), P(), up_spec, up_spec, down_spec, down_spec),
        check_vma=False,
    )
```
